32 devices in a mesh: dp: 2 (over x), expert: 16 (over z, y, core).
Axes of the slice: x: 2, y: 2, z: 4, core: 2. Of those that a mesh axis runs over, the one named last changes fastest.
Arguments:
- tokens: bfloat16 [512, 2048], P('expert', 'dp'), may hold values from -6 to 6
- routes: int32 [512, 8], P('expert'), may hold values from 0 to 63, all different within a row; in each aligned block of 32 rows (0 to 31, 32 to 63, ...) at most 4 rows name the same one
- route_weight: float32 [512, 8], P('expert'), may hold values from 0.05 to 0.5
- gate_weight: bfloat16 [64, 2048, 768], P('expert', 'dp'), may hold values from -0.125 to 0.125
- up_weight: bfloat16 [64, 2048, 768], P('expert', 'dp'), may hold values from -0.125 to 0.125
- down_weight: bfloat16 [64, 768, 2048], P('expert', None, 'dp'), may hold values from -0.21875 to 0.21875
- trained_down: float32 [64, 768, 2048], P('expert', 'dp'), may hold values from -0.21875 to 0.21875
Outputs:
- mixed: bfloat16 [512, 2048], P('expert', 'dp')
- synced_down: bfloat16 [64, 768, 2048], P('expert', None, 'dp')
The draws below stay inside these ranges and needn't reach their ends.
Inputs may be any that keep to these rules, and one draw needn't show every extreme that they name: `routes`: each row names 8 different experts. Among the 32 rows of one device (aligned blocks), no expert is named more than 4 times, a bound that some block reaches.
All inputs are finite; a program needn't handle non-finite values.
Results may differ from the reference program's by a relative error of at most 0.0058.
Values may be sent and summed in bfloat16 or wider, within the bound.
A program may use at most 128 MiB of HBM per device.

```python
import math
import jax
import jax.numpy as jnp
import numpy as np
from jax import lax

D = 2048
FF = 768
TOP = 8
EXPERTS = 64
TOK_DEV = 32
CAP = 4
TOKENS = 512


def level_of(stream_key, extent, pieces, least, high):
    loudness = 1.0
    for dim, parts in pieces:
        heights = jax.random.uniform(jax.random.fold_in(jax.random.fold_in(stream_key, 6), dim), (parts,), jnp.float32, least / len(pieces), high / len(pieces))
        loudness = loudness * jnp.repeat(jnp.exp(heights), extent[dim] // parts).reshape((-1,) + (1,) * (len(extent) - 1 - dim))
    return loudness


def routed_block(key, own, number, rows, amount, top, limit, lean):
    order = jax.random.permutation(key, amount)
    crowded, common = shares(amount, rows * top, limit, lean, True), shares(amount, rows * top, limit, lean, False)
    places = jnp.arange(amount)

    def named(lengths, turn):
        used = int((lengths > 0).sum())
        fixed = max(1, used // 4)
        shifted = fixed + (places - fixed + turn * (used - fixed)) % max(1, amount - fixed)
        return jnp.zeros((amount,), jnp.int32).at[order[jnp.where(places < fixed, places, shifted)]].set(jnp.asarray(lengths, jnp.int32))

    lengths = jnp.where(number % 4 == 0, named(crowded, number // 4), named(common, number - number // 4 - 1))
    mixed = jax.random.permutation(jax.random.fold_in(own, 3), amount)
    giver, receiver = mixed[0:amount // 2 * 2:2], mixed[1:amount // 2 * 2:2]
    margin = jnp.minimum(lengths[giver] - 1, limit - lengths[receiver]) // 2
    margin = jnp.where((giver == order[0]) | (receiver == order[0]) | (lengths[receiver] == 0), 0, jnp.maximum(margin, 0))
    shifted = jax.random.randint(jax.random.fold_in(own, 4), (amount // 2,), 0, 1 << 20) % (margin + 1)
    lengths = lengths.at[giver].add(-shifted).at[receiver].add(shifted)
    items = jnp.searchsorted(jnp.cumsum(lengths), jnp.arange(rows * top), side="right").astype(jnp.int32)
    grid = items.reshape(top, rows).T
    grid = grid[jax.random.permutation(jax.random.fold_in(own, 1), rows)]
    turn = jax.random.randint(jax.random.fold_in(own, 2), (rows, 1), 0, top)
    return jnp.take_along_axis(grid, (jnp.arange(top)[None, :] + turn) % top, axis=1)


def shares(number_of, total, most, slope, full):
    loads = [(1 << 20) // math.isqrt(standing ** slope) + 1 for standing in range(1, number_of + 1)]
    largest = most if full else min(most, max(-(-total // number_of), total * loads[0] // sum(loads)))
    least = 1 if total - largest >= number_of - 1 else 0
    given, spare = [largest] + [least] * (number_of - 1), total - largest - least * (number_of - 1)
    while spare > 0:
        movable = [i for i in range(1, number_of) if given[i] < largest] or [i for i in range(1, number_of) if given[i] < most]
        pool, remaining = sum([loads[i] for i in movable]), spare
        for i in movable:
            addition = min(most - given[i], max(1, remaining * loads[i] // pool), spare)
            given[i] = given[i] + addition
            spare = spare - addition
    return np.array(given)


def noise(key, extent, width, reach, split=(), kind=jnp.bfloat16):
    loudness = level_of(key, extent, split, -0.22, 0.18) if split else 1.0
    drawn = jax.random.normal(key, extent, jnp.float32) * width * loudness
    return jnp.minimum(jnp.maximum(drawn, -reach), reach).astype(kind)


def setup_inputs(seed: int = 0) -> dict:
    key_list = jax.random.split(jax.random.key(seed), 8)
    tokens = noise(key_list[0], (TOKENS, D), 1.0, 6.0, ((0, 16), (1, 2)))
    routes_keys = jax.random.split(jax.random.fold_in(key_list[1], 1), TOKENS // TOK_DEV)
    routes_turns = jax.random.permutation(jax.random.fold_in(key_list[1], 3), TOKENS // TOK_DEV)
    routes = jax.vmap(lambda own, number: routed_block(jax.random.fold_in(key_list[1], 2), own, number, TOK_DEV, EXPERTS, TOP, CAP, 2))(routes_keys, routes_turns).reshape((TOKENS, TOP))
    route_weight = jnp.clip(jnp.exp(math.log(0.5) - 2.3025851 * jax.random.uniform(key_list[2], (TOKENS, TOP), jnp.float32) ** level_of(key_list[2], (TOKENS, TOP), ((0, 16),), -0.2, 0.2)), 0.05, 0.5)
    gate_weight = noise(key_list[3], (EXPERTS, D, FF), D ** -0.5, 0.125, ((0, 16), (1, 2)))
    up_weight = noise(key_list[4], (EXPERTS, D, FF), D ** -0.5, 0.125, ((0, 16), (1, 2)))
    down_weight = noise(key_list[5], (EXPERTS, FF, D), FF ** -0.5, 0.21875, ((0, 16), (2, 2)))
    trained_down = noise(key_list[6], (EXPERTS, FF, D), FF ** -0.5, 0.21875, ((0, 16), (1, 2)), jnp.float32)
    return {"tokens": tokens, "routes": routes, "route_weight": route_weight, "gate_weight": gate_weight, "up_weight": up_weight, "down_weight": down_weight, "trained_down": trained_down}


def reference(tokens, routes, route_weight, gate_weight, up_weight, down_weight, trained_down):
    blocks = TOKENS // TOK_DEV
    labels = jnp.arange(EXPERTS, dtype=jnp.int32)
    counts = jnp.sum((routes[:, :, None] == labels[None, None, :]).astype(jnp.int32), axis=1)
    per_block = counts.reshape(blocks, TOK_DEV, EXPERTS)
    earlier = (jnp.cumsum(per_block, axis=1) - per_block).reshape(TOKENS, EXPERTS).astype(jnp.int32)
    slot_index = jnp.take_along_axis(earlier, routes, axis=1).astype(jnp.int32)
    block_of = (jnp.arange(TOKENS, dtype=jnp.int32) // TOK_DEV)[:, None]
    position = (block_of * CAP + slot_index).astype(jnp.int32)
    rows_expert = blocks * CAP
    token_ids = jnp.broadcast_to(jnp.arange(TOKENS, dtype=jnp.int32)[:, None], routes.shape)
    row_table = jnp.full((EXPERTS, rows_expert), TOKENS, jnp.int32).at[routes, position].set(token_ids)
    padded = jnp.concatenate([tokens, jnp.zeros((1, D), tokens.dtype)], axis=0)

    def one_expert(operands):
        row_index, gate_mat, up_mat, down_mat = operands
        gathered = padded[row_index]
        gate_pre = jnp.dot(gathered, gate_mat, preferred_element_type=jnp.float32)
        up_pre = jnp.dot(gathered, up_mat, preferred_element_type=jnp.float32)
        hidden = (jax.nn.silu(gate_pre) * up_pre).astype(jnp.bfloat16)
        return jnp.dot(hidden, down_mat, preferred_element_type=jnp.float32).astype(jnp.bfloat16)

    results = lax.map(one_expert, (row_table, gate_weight, up_weight, down_weight))
    picked = results[routes, position]
    mixed = jnp.sum(route_weight[:, :, None] * picked.astype(jnp.float32), axis=1).astype(jnp.bfloat16)
    return mixed, trained_down.astype(jnp.bfloat16)
```

```python
import functools

import jax
import jax.numpy as jnp
from jax import lax
from jax.experimental import pallas as pl
from jax.experimental.pallas import tpu as pltpu
from jax.sharding import PartitionSpec as P

CAP = 4
CHUNK_BYTES = 200_000
FIRST = 2
EARLY = 5 / 16
MIDDLE = 1 / 16
LATE = 1 / 4
MESH = pl.DeviceIdType.MESH


def each(start, stop, body):
    def step(i, carry):
        body(i)
        return carry

    lax.fori_loop(start, stop, step, 0)


def chunk_at(dims, i):
    n, _, el, rc, nsub, _ = dims
    offset = lax.rem(lax.div(i, el * nsub) + 1, n)
    e = lax.rem(lax.div(i, nsub), el)
    return offset, e, lax.rem(i, nsub) * rc


def rows_of(dims, rows, source, r):
    return pl.ds(pl.multiple_of(source * rows + r, 16), dims[3])


def fused(
    dims,
    tokens, routes, route_weight, gate_weight, up_weight, down_weight, trained,
    mixed, synced,
    tok_v, routes_v, weight_v, gate_v, up_v, down_v, wide, narrow,
    outgoing, arrived, by_expert, partial, to_send, peers_part, hidden,
    leaving, returned,
    small_sem, load_sem, wide_sem, sync_send, sync_recv,
    out_send, out_recv, part_send, part_recv, hid_send, hid_recv, ret_send, ret_recv,
    entered,
):
    n, groups, el, rc, nsub, late = dims
    p, me = lax.axis_index("dp"), lax.axis_index("expert")
    core = lax.rem(me, 2)
    rows = trained.shape[1]
    tok_rows, width = tok_v.shape
    ff = gate_v.shape[2]
    slots = el * CAP
    total = groups * slots
    share = total // n
    per_expert = total // el
    per_peer = el * nsub
    remote = (n - 1) * per_peer
    early = round(remote * EARLY)
    middle = early + round(remote * MIDDLE)
    own = remote - core * late

    def peer(offset):
        return lax.rem(p + offset, n)

    def share_of(device):
        return pl.ds(pl.multiple_of(device * share, 16), share)

    def load_wide(i):
        offset, e, r = chunk_at(dims, i)
        cols = pl.ds(pl.multiple_of(peer(offset) * width, 128), width)
        return pltpu.make_async_copy(
            trained.at[e, pl.ds(pl.multiple_of(r, 16), rc), cols], wide.at[i], wide_sem.at[i]
        )

    def sync_copy(i):
        offset, e, r = chunk_at(dims, i)
        return pltpu.make_async_remote_copy(
            src_ref=narrow.at[i],
            dst_ref=synced.at[e, rows_of(dims, rows, p, r), :],
            send_sem=sync_send.at[i],
            recv_sem=sync_recv.at[i],
            device_id=(peer(offset), me),
            device_id_type=MESH,
        )

    def sync_arrival(i):
        offset, e, r = chunk_at(dims, i)
        source = lax.rem(p + n - offset, n)
        return pltpu.make_async_remote_copy(
            src_ref=narrow.at[i],
            dst_ref=synced.at[e, rows_of(dims, rows, source, r), :],
            send_sem=sync_send.at[i],
            recv_sem=sync_recv.at[i],
            device_id=(peer(offset), me),
            device_id_type=MESH,
        )

    def send_chunk(i):
        load_wide(i).wait()
        narrow[i] = wide[i].astype(jnp.bfloat16)
        sync_copy(i).start()

    def spread(source, target, send, recv, offset, slot):
        return pltpu.make_async_remote_copy(
            src_ref=source.at[slot],
            dst_ref=target.at[me],
            send_sem=send.at[offset],
            recv_sem=recv.at[offset],
            device_id=(p, slot),
            device_id_type=MESH,
        )

    def spread_all(source, target, send, recv):
        each(
            1, groups,
            lambda o: spread(source, target, send, recv, o, lax.rem(me + o, groups)).start(),
        )

    def gather_all(source, target, send, recv):
        def body(o):
            origin = lax.rem(me + groups - o, groups)
            pltpu.make_async_remote_copy(
                src_ref=source.at[origin],
                dst_ref=target.at[origin],
                send_sem=send.at[o],
                recv_sem=recv.at[o],
                device_id=(p, origin),
                device_id_type=MESH,
            ).wait_recv()

        each(1, groups, body)

    def part_copy(o):
        return pltpu.make_async_remote_copy(
            src_ref=to_send.at[peer(o)],
            dst_ref=peers_part.at[o],
            send_sem=part_send.at[o],
            recv_sem=part_recv.at[o],
            device_id=(peer(o), me),
            device_id_type=MESH,
        )

    def hidden_copy(o, origin):
        return pltpu.make_async_remote_copy(
            src_ref=hidden.at[share_of(origin), :],
            dst_ref=hidden.at[share_of(origin), :],
            send_sem=hid_send.at[o],
            recv_sem=hid_recv.at[o],
            device_id=(peer(o), me),
            device_id_type=MESH,
        )

    smalls = [
        pltpu.make_async_copy(src, dst, small_sem.at[i])
        for i, (src, dst) in enumerate(
            ((routes, routes_v), (route_weight, weight_v), (tokens, tok_v))
        )
    ]

    def weights(k, src, dst):
        return lambda e: pltpu.make_async_copy(src.at[e], dst.at[e], load_sem.at[k * el + e])

    load_gate = weights(0, gate_weight, gate_v)
    load_up = weights(1, up_weight, up_v)
    load_down = weights(2, down_weight, down_v)

    barrier = pltpu.get_barrier_semaphore()

    def greet(device):
        pl.semaphore_signal(barrier, inc=1, device_id=device, device_id_type=MESH)

    leader = me - core
    each(1, n, lambda o: greet((peer(o), me)))

    @pl.when(core == 0)
    def _():
        greet((p, me + 1))

    @pl.when(core == 1)
    def _():
        each(0, groups // 2, lambda j: greet((p, lax.rem(leader + 2 * j, groups))))

    @pl.when(core == 0)
    def _():
        each(1, groups // 2, lambda j: greet((p, lax.rem(leader + 2 * j, groups))))

    each(0, FIRST, lambda i: load_wide(i).start())
    for copy in smalls:
        copy.start()
    each(FIRST, early, lambda i: load_wide(i).start())
    each(0, el, lambda e: load_gate(e).start())
    each(0, el, lambda e: load_up(e).start())
    each(early, own, lambda i: load_wide(i).start())
    each(0, el, lambda e: load_down(e).start())
    each(remote, remote + per_peer, lambda i: load_wide(i).start())
    pl.semaphore_wait(barrier, n - 1 + jnp.where(core == 0, groups - 1, 1))

    @pl.when(core == 0)
    def _():
        pl.semaphore_signal(entered, inc=1, device_id=(p, me + 1), device_id_type=MESH)

    each(0, FIRST, send_chunk)

    for copy in smalls:
        copy.wait()
    slot = lax.broadcasted_iota(jnp.int32, (total, tok_rows), 0)
    slot_expert = slot // CAP
    chosen = jnp.zeros((total, tok_rows), jnp.float32)
    scale = jnp.zeros((total, tok_rows), jnp.float32)
    for k in range(routes_v.shape[0]):
        hit = routes_v[k : k + 1, :] == slot_expert
        chosen = chosen + jnp.where(hit, 1.0, 0.0)
        scale = scale + jnp.where(hit, weight_v[k : k + 1, :], 0.0)
    row = lax.broadcasted_iota(jnp.int32, (tok_rows, tok_rows), 0)
    col = lax.broadcasted_iota(jnp.int32, (tok_rows, tok_rows), 1)
    before = jnp.where(row < col, 1.0, 0.0).astype(jnp.bfloat16)
    earlier = jnp.dot(chosen.astype(jnp.bfloat16), before, preferred_element_type=jnp.float32)
    placed = (chosen == 1.0) & (earlier == (slot % CAP).astype(jnp.float32))
    combine = jnp.where(placed, scale, 0.0).T
    dispatch = jnp.where(placed, 1.0, 0.0).astype(jnp.bfloat16)
    outgoing[...] = (
        jnp.dot(dispatch, tok_v[...], preferred_element_type=jnp.float32)
        .astype(jnp.bfloat16)
        .reshape(groups, slots, width)
    )
    arrived[me] = outgoing[me]

    @pl.when(core == 1)
    def _():
        pl.semaphore_wait(entered, 1)

    spread_all(outgoing, arrived, out_send, out_recv)
    each(FIRST, early, send_chunk)

    r = lax.broadcasted_iota(jnp.int32, (total, total), 0)
    c = lax.broadcasted_iota(jnp.int32, (total, total), 1)
    home = ((r // CAP) % groups) * slots + (r // per_expert) * CAP + r % CAP
    order = jnp.where(c == home, 1.0, 0.0)
    gather_all(outgoing, arrived, out_send, out_recv)
    by_expert[...] = (
        jnp.dot(
            order.astype(jnp.bfloat16),
            arrived[...].reshape(total, width),
            preferred_element_type=jnp.float32,
        )
        .astype(jnp.bfloat16)
        .reshape(el, per_expert, width)
    )

    def project(e):
        load_gate(e).wait()
        load_up(e).wait()
        x = by_expert[e]
        at = pl.ds(pl.multiple_of(e * per_expert, 16), per_expert)
        partial[at, :ff] = jnp.dot(x, gate_v[e], preferred_element_type=jnp.float32)
        partial[at, ff:] = jnp.dot(x, up_v[e], preferred_element_type=jnp.float32)

    each(0, el, project)
    to_send[...] = partial[...].reshape(n, share, 2 * ff).astype(jnp.bfloat16)
    each(1, n, lambda o: part_copy(o).start())
    each(early, middle, send_chunk)

    each(1, n, lambda o: part_copy(o).wait_recv())

    def gather_part(o, acc):
        return acc + peers_part[o].astype(jnp.float32)

    summed = lax.fori_loop(1, n, gather_part, partial[share_of(p), :])
    gate, up = summed[:, :ff], summed[:, ff:]
    hidden[share_of(p), :] = (gate / (1.0 + jnp.exp(-gate)) * up).astype(jnp.bfloat16)
    each(1, n, lambda o: hidden_copy(o, p).start())
    each(middle, own, send_chunk)
    each(1, n, lambda o: hidden_copy(o, lax.rem(p + n - o, n)).wait_recv())

    def contract(e):
        load_down(e).wait()
        h = hidden[pl.ds(pl.multiple_of(e * per_expert, 16), per_expert), :]
        by_expert[e] = jnp.dot(h, down_v[e], preferred_element_type=jnp.float32).astype(
            jnp.bfloat16
        )

    each(0, el, contract)
    leaving[...] = (
        jnp.dot(
            order.T.astype(jnp.bfloat16),
            by_expert[...].reshape(total, width),
            preferred_element_type=jnp.float32,
        )
        .astype(jnp.bfloat16)
        .reshape(groups, slots, width)
    )
    returned[me] = leaving[me]
    spread_all(leaving, returned, ret_send, ret_recv)

    def keep(i):
        load_wide(i).wait()
        _, e, r = chunk_at(dims, i)
        synced[e, rows_of(dims, rows, p, r), :] = wide[i].astype(jnp.bfloat16)

    each(remote, remote + per_peer, keep)
    gather_all(leaving, returned, ret_send, ret_recv)
    answers = returned[...].reshape(total, width)
    high = combine.astype(jnp.bfloat16)
    rest = combine - high.astype(jnp.float32)
    mid = rest.astype(jnp.bfloat16)
    low = (rest - mid.astype(jnp.float32)).astype(jnp.bfloat16)
    mixed[...] = (
        jnp.dot(low, answers, preferred_element_type=jnp.float32)
        + jnp.dot(mid, answers, preferred_element_type=jnp.float32)
        + jnp.dot(high, answers, preferred_element_type=jnp.float32)
    ).astype(jnp.bfloat16)

    each(
        1, groups,
        lambda o: spread(
            outgoing, arrived, out_send, out_recv, o, lax.rem(me + o, groups)
        ).wait_send(),
    )
    each(
        1, groups,
        lambda o: spread(
            leaving, returned, ret_send, ret_recv, o, lax.rem(me + o, groups)
        ).wait_send(),
    )
    each(1, n, lambda o: part_copy(o).wait_send())
    each(1, n, lambda o: hidden_copy(o, p).wait_send())

    def finish(i):
        sync_copy(i).wait_send()
        sync_arrival(i).wait_recv()

    each(0, own, finish)


def store(dims, mixed, synced, mixed_out, synced_out, mark, sems):
    n, _, el, _, nsub, late = dims
    p, core = lax.axis_index("dp"), lax.rem(lax.axis_index("expert"), 2)
    rows = synced.shape[1] // n
    own = (n - 1) * el * nsub - core * late

    def local_part(e):
        part = pl.ds(pl.multiple_of(p * rows, 16), rows)
        return pltpu.make_async_copy(synced.at[e, part], synced_out.at[e, part], sems.at[e])

    def arrived_part(i):
        offset, e, r = chunk_at(dims, i)
        part = rows_of(dims, rows, lax.rem(p + n - offset, n), r)
        return pltpu.make_async_copy(synced.at[e, part], synced_out.at[e, part], sems.at[el + i])

    out = pltpu.make_async_copy(mixed, mixed_out, sems.at[sems.shape[0] - 1])
    each(0, el, lambda e: local_part(e).start())
    each(0, own, lambda i: arrived_part(i).start())
    out.start()
    mark[...] = jnp.zeros_like(mark)
    each(0, el, lambda e: local_part(e).wait())
    each(0, own, lambda i: arrived_part(i).wait())
    out.wait()


def trailing(dims, trained, mark, tail, wide, narrow, wide_sem, send_sem, recv_sem):
    n, _, el, rc, nsub, late = dims
    p, me = lax.axis_index("dp"), lax.axis_index("expert")
    width = wide.shape[2]
    first = (n - 1) * el * nsub - late
    stop = lax.rem(me, 2) * late

    def load(i):
        offset, e, r = chunk_at(dims, first + i)
        cols = pl.ds(pl.multiple_of(lax.rem(p + offset, n) * width, 128), width)
        return pltpu.make_async_copy(
            trained.at[e, pl.ds(pl.multiple_of(r, 16), rc), cols], wide.at[i], wide_sem.at[i]
        )

    def copy(i):
        offset, _, _ = chunk_at(dims, first + i)
        return pltpu.make_async_remote_copy(
            src_ref=narrow.at[i],
            dst_ref=tail.at[i],
            send_sem=send_sem.at[i],
            recv_sem=recv_sem.at[i],
            device_id=(lax.rem(p + offset, n), me),
            device_id_type=MESH,
        )

    def send(i):
        load(i).wait()
        narrow[i] = wide[i].astype(jnp.bfloat16)
        copy(i).start()

    barrier = pltpu.get_barrier_semaphore()
    each(
        1, n,
        lambda o: pl.semaphore_signal(
            barrier, inc=1, device_id=(lax.rem(p + o, n), me), device_id_type=MESH
        ),
    )
    each(0, stop, lambda i: load(i).start())
    pl.semaphore_wait(barrier, n - 1)
    each(0, stop, send)
    each(0, stop, lambda i: copy(i).wait())


def settle(dims, tail, stored, synced_out, sems):
    n, _, el, _, nsub, late = dims
    p, core = lax.axis_index("dp"), lax.rem(lax.axis_index("expert"), 2)
    rows = synced_out.shape[1] // n
    first = (n - 1) * el * nsub - late

    def part(i):
        offset, e, r = chunk_at(dims, first + i)
        source = lax.rem(p + n - offset, n)
        return pltpu.make_async_copy(
            tail.at[i], synced_out.at[e, rows_of(dims, rows, source, r)], sems.at[i]
        )

    each(0, core * late, lambda i: part(i).start())
    each(0, core * late, lambda i: part(i).wait())


def local(tokens, routes, route_weight, gate_weight, up_weight, down_weight, trained_down):
    n, groups = lax.axis_size("dp"), lax.axis_size("expert")
    tok_rows, width = tokens.shape
    el, _, ff = gate_weight.shape
    rows = trained_down.shape[1]
    slots = el * CAP
    total = groups * slots
    share = total // n
    fits = [
        d for d in range(16, rows + 1, 16) if rows % d == 0 and d * width * 2 <= CHUNK_BYTES
    ]
    rc = fits[-1]
    nsub = rows // rc
    chunks = n * el * nsub
    remote = chunks - el * nsub
    late = round(remote * LATE)
    dims = (n, groups, el, rc, nsub, late)
    bf16, f32 = jnp.bfloat16, jnp.float32
    inside = pl.BlockSpec(memory_space=pltpu.VMEM)
    anywhere = pl.BlockSpec(memory_space=pl.ANY)
    dma = pltpu.SemaphoreType.DMA
    routes, route_weight = routes.T, route_weight.T

    def in_vmem(x):
        return pltpu.with_memory_space_constraint(x, pltpu.VMEM)

    mixed, synced = pl.pallas_call(
        functools.partial(fused, dims),
        out_shape=(
            pltpu.VMEM((tok_rows, width), bf16),
            pltpu.VMEM((el, n * rows, width), bf16),
        ),
        in_specs=[anywhere] * 7,
        out_specs=(inside, inside),
        scratch_shapes=[
            pltpu.VMEM(tokens.shape, bf16),
            pltpu.VMEM(routes.shape, jnp.int32),
            pltpu.VMEM(route_weight.shape, f32),
            pltpu.VMEM(gate_weight.shape, bf16),
            pltpu.VMEM(up_weight.shape, bf16),
            pltpu.VMEM(down_weight.shape, bf16),
            pltpu.VMEM((chunks, rc, width), f32),
            pltpu.VMEM((remote, rc, width), bf16),
            pltpu.VMEM((groups, slots, width), bf16),
            pltpu.VMEM((groups, slots, width), bf16),
            pltpu.VMEM((el, total // el, width), bf16),
            pltpu.VMEM((total, 2 * ff), f32),
            pltpu.VMEM((n, share, 2 * ff), bf16),
            pltpu.VMEM((n, share, 2 * ff), bf16),
            pltpu.VMEM((total, ff), bf16),
            pltpu.VMEM((groups, slots, width), bf16),
            pltpu.VMEM((groups, slots, width), bf16),
            dma((3,)),
            dma((3 * el,)),
            dma((chunks,)),
            dma((remote,)),
            dma((remote,)),
            dma((groups,)),
            dma((groups,)),
            dma((n,)),
            dma((n,)),
            dma((n,)),
            dma((n,)),
            dma((groups,)),
            dma((groups,)),
            pltpu.SemaphoreType.REGULAR,
        ],
        compiler_params=pltpu.CompilerParams(
            collective_id=0, has_side_effects=True, vmem_limit_bytes=52 * 2**20
        ),
        cost_estimate=pl.CostEstimate(
            flops=6 * total * width * ff, bytes_accessed=2**28, transcendentals=0
        ),
    )(tokens, routes, route_weight, gate_weight, up_weight, down_weight, trained_down)
    mixed, stored, mark = pl.pallas_call(
        functools.partial(store, dims),
        out_shape=(
            jax.ShapeDtypeStruct((tok_rows, width), bf16),
            jax.ShapeDtypeStruct((el, n * rows, width), bf16),
            pltpu.VMEM((8, 128), f32),
        ),
        in_specs=[inside] * 2,
        out_specs=(anywhere, anywhere, inside),
        scratch_shapes=[dma((el + remote + 1,))],
        compiler_params=pltpu.CompilerParams(vmem_limit_bytes=2**20),
    )(in_vmem(mixed), in_vmem(synced))
    tail = pl.pallas_call(
        functools.partial(trailing, dims),
        out_shape=pltpu.VMEM((late, rc, width), bf16),
        in_specs=[anywhere] * 2,
        out_specs=inside,
        scratch_shapes=[
            pltpu.VMEM((late, rc, width), f32),
            pltpu.VMEM((late, rc, width), bf16),
            dma((late,)),
            dma((late,)),
            dma((late,)),
        ],
        compiler_params=pltpu.CompilerParams(
            collective_id=1, has_side_effects=True, vmem_limit_bytes=56 * 2**20
        ),
    )(trained_down, in_vmem(mark))
    synced = pl.pallas_call(
        functools.partial(settle, dims),
        out_shape=jax.ShapeDtypeStruct((el, n * rows, width), bf16),
        in_specs=[inside, anywhere],
        out_specs=anywhere,
        scratch_shapes=[dma((late,))],
        input_output_aliases={1: 0},
        compiler_params=pltpu.CompilerParams(vmem_limit_bytes=2**20),
    )(in_vmem(tail), stored)
    return mixed, synced


def solution(mesh):
    placed = (
        P("expert", "dp"),
        P("expert", None),
        P("expert", None),
        P("expert", "dp", None),
        P("expert", "dp", None),
        P("expert", None, "dp"),
        P("expert", "dp", None),
    )
    return jax.shard_map(
        local,
        mesh=mesh,
        in_specs=placed,
        out_specs=(P("expert", "dp"), P("expert", None, "dp")),
        check_vma=False,
    )
```

```python
import functools

import jax
import jax.numpy as jnp
from jax import lax
from jax.experimental import pallas as pl
from jax.experimental.pallas import tpu as pltpu
from jax.sharding import PartitionSpec as P

CAP = 4
CHUNK_BYTES = 200_000
FIRST = 2
EARLY = 5 / 16
MIDDLE = 1 / 16
LATE = 3 / 16
COVER = 4
MESH = pl.DeviceIdType.MESH


def each(start, stop, body):
    def step(i, carry):
        body(i)
        return carry

    lax.fori_loop(start, stop, step, 0)


def chunk_at(dims, i):
    n, _, el, rc, nsub, _ = dims
    offset = lax.rem(lax.div(i, el * nsub) + 1, n)
    e = lax.rem(lax.div(i, nsub), el)
    return offset, e, lax.rem(i, nsub) * rc


def rows_of(dims, rows, source, r):
    return pl.ds(pl.multiple_of(source * rows + r, 16), dims[3])


def fused(
    dims,
    tokens, routes, route_weight, gate_weight, up_weight, down_weight, trained,
    mixed, synced,
    tok_v, routes_v, weight_v, gate_v, up_v, down_v, wide, narrow,
    outgoing, arrived, by_expert, partial, to_send, peers_part, hidden,
    leaving, returned,
    small_sem, load_sem, wide_sem, sync_send, sync_recv,
    out_send, out_recv, part_send, part_recv, hid_send, hid_recv, ret_send, ret_recv,
    entered, nearly,
):
    n, groups, el, rc, nsub, late = dims
    p, me = lax.axis_index("dp"), lax.axis_index("expert")
    core = lax.rem(me, 2)
    rows = trained.shape[1]
    tok_rows, width = tok_v.shape
    ff = gate_v.shape[2]
    slots = el * CAP
    total = groups * slots
    share = total // n
    per_expert = total // el
    per_peer = el * nsub
    remote = (n - 1) * per_peer
    early = round(remote * EARLY)
    middle = early + round(remote * MIDDLE)
    own = remote - core * late

    def peer(offset):
        return lax.rem(p + offset, n)

    def share_of(device):
        return pl.ds(pl.multiple_of(device * share, 16), share)

    def load_wide(i):
        offset, e, r = chunk_at(dims, i)
        cols = pl.ds(pl.multiple_of(peer(offset) * width, 128), width)
        return pltpu.make_async_copy(
            trained.at[e, pl.ds(pl.multiple_of(r, 16), rc), cols], wide.at[i], wide_sem.at[i]
        )

    def sync_copy(i):
        offset, e, r = chunk_at(dims, i)
        return pltpu.make_async_remote_copy(
            src_ref=narrow.at[i],
            dst_ref=synced.at[e, rows_of(dims, rows, p, r), :],
            send_sem=sync_send.at[i],
            recv_sem=sync_recv.at[i],
            device_id=(peer(offset), me),
            device_id_type=MESH,
        )

    def sync_arrival(i):
        offset, e, r = chunk_at(dims, i)
        source = lax.rem(p + n - offset, n)
        return pltpu.make_async_remote_copy(
            src_ref=narrow.at[i],
            dst_ref=synced.at[e, rows_of(dims, rows, source, r), :],
            send_sem=sync_send.at[i],
            recv_sem=sync_recv.at[i],
            device_id=(peer(offset), me),
            device_id_type=MESH,
        )

    def send_chunk(i):
        load_wide(i).wait()
        narrow[i] = wide[i].astype(jnp.bfloat16)
        sync_copy(i).start()

    def spread(source, target, send, recv, offset, slot):
        return pltpu.make_async_remote_copy(
            src_ref=source.at[slot],
            dst_ref=target.at[me],
            send_sem=send.at[offset],
            recv_sem=recv.at[offset],
            device_id=(p, slot),
            device_id_type=MESH,
        )

    def spread_all(source, target, send, recv):
        each(
            1, groups,
            lambda o: spread(source, target, send, recv, o, lax.rem(me + o, groups)).start(),
        )

    def gather_all(source, target, send, recv):
        def body(o):
            origin = lax.rem(me + groups - o, groups)
            pltpu.make_async_remote_copy(
                src_ref=source.at[origin],
                dst_ref=target.at[origin],
                send_sem=send.at[o],
                recv_sem=recv.at[o],
                device_id=(p, origin),
                device_id_type=MESH,
            ).wait_recv()

        each(1, groups, body)

    def part_copy(o):
        return pltpu.make_async_remote_copy(
            src_ref=to_send.at[peer(o)],
            dst_ref=peers_part.at[o],
            send_sem=part_send.at[o],
            recv_sem=part_recv.at[o],
            device_id=(peer(o), me),
            device_id_type=MESH,
        )

    def hidden_copy(o, origin):
        return pltpu.make_async_remote_copy(
            src_ref=hidden.at[share_of(origin), :],
            dst_ref=hidden.at[share_of(origin), :],
            send_sem=hid_send.at[o],
            recv_sem=hid_recv.at[o],
            device_id=(peer(o), me),
            device_id_type=MESH,
        )

    smalls = [
        pltpu.make_async_copy(src, dst, small_sem.at[i])
        for i, (src, dst) in enumerate(
            ((routes, routes_v), (route_weight, weight_v), (tokens, tok_v))
        )
    ]

    def weights(k, src, dst):
        return lambda e: pltpu.make_async_copy(src.at[e], dst.at[e], load_sem.at[k * el + e])

    load_gate = weights(0, gate_weight, gate_v)
    load_up = weights(1, up_weight, up_v)
    load_down = weights(2, down_weight, down_v)

    barrier = pltpu.get_barrier_semaphore()

    def greet(device):
        pl.semaphore_signal(barrier, inc=1, device_id=device, device_id_type=MESH)

    each(0, FIRST, lambda i: load_wide(i).start())
    leader = me - core
    each(1, n, lambda o: greet((peer(o), me)))

    @pl.when(core == 0)
    def _():
        greet((p, me + 1))

    @pl.when(core == 1)
    def _():
        each(0, groups // 2, lambda j: greet((p, lax.rem(leader + 2 * j, groups))))

    @pl.when(core == 0)
    def _():
        each(1, groups // 2, lambda j: greet((p, lax.rem(leader + 2 * j, groups))))

    for copy in smalls:
        copy.start()
    each(FIRST, early, lambda i: load_wide(i).start())
    each(0, el, lambda e: load_gate(e).start())
    each(0, el, lambda e: load_up(e).start())
    each(early, own, lambda i: load_wide(i).start())
    each(0, el, lambda e: load_down(e).start())
    each(remote, remote + per_peer, lambda i: load_wide(i).start())
    pl.semaphore_wait(barrier, n - 1 + jnp.where(core == 0, groups - 1, 1))

    @pl.when(core == 0)
    def _():
        pl.semaphore_signal(entered, inc=1, device_id=(p, me + 1), device_id_type=MESH)

    each(0, FIRST, send_chunk)

    for copy in smalls:
        copy.wait()
    slot = lax.broadcasted_iota(jnp.int32, (total, tok_rows), 0)
    slot_expert = slot // CAP
    chosen = jnp.zeros((total, tok_rows), jnp.float32)
    scale = jnp.zeros((total, tok_rows), jnp.float32)
    for k in range(routes_v.shape[0]):
        hit = routes_v[k : k + 1, :] == slot_expert
        chosen = chosen + jnp.where(hit, 1.0, 0.0)
        scale = scale + jnp.where(hit, weight_v[k : k + 1, :], 0.0)
    row = lax.broadcasted_iota(jnp.int32, (tok_rows, tok_rows), 0)
    col = lax.broadcasted_iota(jnp.int32, (tok_rows, tok_rows), 1)
    before = jnp.where(row < col, 1.0, 0.0).astype(jnp.bfloat16)
    earlier = jnp.dot(chosen.astype(jnp.bfloat16), before, preferred_element_type=jnp.float32)
    placed = (chosen == 1.0) & (earlier == (slot % CAP).astype(jnp.float32))
    combine = jnp.where(placed, scale, 0.0).T
    dispatch = jnp.where(placed, 1.0, 0.0).astype(jnp.bfloat16)
    outgoing[...] = (
        jnp.dot(dispatch, tok_v[...], preferred_element_type=jnp.float32)
        .astype(jnp.bfloat16)
        .reshape(groups, slots, width)
    )
    arrived[me] = outgoing[me]

    @pl.when(core == 1)
    def _():
        pl.semaphore_wait(entered, 1)

    spread_all(outgoing, arrived, out_send, out_recv)
    each(FIRST, early, send_chunk)

    r = lax.broadcasted_iota(jnp.int32, (total, total), 0)
    c = lax.broadcasted_iota(jnp.int32, (total, total), 1)
    home = ((r // CAP) % groups) * slots + (r // per_expert) * CAP + r % CAP
    order = jnp.where(c == home, 1.0, 0.0)
    gather_all(outgoing, arrived, out_send, out_recv)
    by_expert[...] = (
        jnp.dot(
            order.astype(jnp.bfloat16),
            arrived[...].reshape(total, width),
            preferred_element_type=jnp.float32,
        )
        .astype(jnp.bfloat16)
        .reshape(el, per_expert, width)
    )

    def project(e):
        load_gate(e).wait()
        load_up(e).wait()
        x = by_expert[e]
        at = pl.ds(pl.multiple_of(e * per_expert, 16), per_expert)
        partial[at, :ff] = jnp.dot(x, gate_v[e], preferred_element_type=jnp.float32)
        partial[at, ff:] = jnp.dot(x, up_v[e], preferred_element_type=jnp.float32)

    each(0, el, project)
    to_send[...] = partial[...].reshape(n, share, 2 * ff).astype(jnp.bfloat16)
    each(1, n, lambda o: part_copy(o).start())
    each(early, middle, send_chunk)

    each(1, n, lambda o: part_copy(o).wait_recv())

    def gather_part(o, acc):
        return acc + peers_part[o].astype(jnp.float32)

    summed = lax.fori_loop(1, n, gather_part, partial[share_of(p), :])
    gate, up = summed[:, :ff], summed[:, ff:]
    hidden[share_of(p), :] = (gate / (1.0 + jnp.exp(-gate)) * up).astype(jnp.bfloat16)
    each(1, n, lambda o: hidden_copy(o, p).start())
    each(middle, own, send_chunk)
    each(1, n, lambda o: hidden_copy(o, lax.rem(p + n - o, n)).wait_recv())

    def contract(e):
        load_down(e).wait()
        h = hidden[pl.ds(pl.multiple_of(e * per_expert, 16), per_expert), :]
        by_expert[e] = jnp.dot(h, down_v[e], preferred_element_type=jnp.float32).astype(
            jnp.bfloat16
        )

    each(0, el, contract)
    leaving[...] = (
        jnp.dot(
            order.T.astype(jnp.bfloat16),
            by_expert[...].reshape(total, width),
            preferred_element_type=jnp.float32,
        )
        .astype(jnp.bfloat16)
        .reshape(groups, slots, width)
    )
    returned[me] = leaving[me]
    spread_all(leaving, returned, ret_send, ret_recv)

    def keep(i):
        load_wide(i).wait()
        _, e, r = chunk_at(dims, i)
        synced[e, rows_of(dims, rows, p, r), :] = wide[i].astype(jnp.bfloat16)

    each(remote, remote + per_peer, keep)
    gather_all(leaving, returned, ret_send, ret_recv)
    answers = returned[...].reshape(total, width)
    high = combine.astype(jnp.bfloat16)
    rest = combine - high.astype(jnp.float32)
    mid = rest.astype(jnp.bfloat16)
    low = (rest - mid.astype(jnp.float32)).astype(jnp.bfloat16)
    mixed[...] = (
        jnp.dot(low, answers, preferred_element_type=jnp.float32)
        + jnp.dot(mid, answers, preferred_element_type=jnp.float32)
        + jnp.dot(high, answers, preferred_element_type=jnp.float32)
    ).astype(jnp.bfloat16)

    each(
        1, groups,
        lambda o: spread(
            outgoing, arrived, out_send, out_recv, o, lax.rem(me + o, groups)
        ).wait_send(),
    )
    each(
        1, groups,
        lambda o: spread(
            leaving, returned, ret_send, ret_recv, o, lax.rem(me + o, groups)
        ).wait_send(),
    )
    each(1, n, lambda o: part_copy(o).wait_send())
    each(1, n, lambda o: hidden_copy(o, p).wait_send())

    def finish(i):
        sync_copy(i).wait_send()
        sync_arrival(i).wait_recv()

    each(0, own - COVER, finish)

    @pl.when(core == 0)
    def _():
        pl.semaphore_signal(nearly, inc=1, device_id=(p, me + 1), device_id_type=MESH)

    each(own - COVER, own, finish)

    @pl.when(core == 1)
    def _():
        pl.semaphore_wait(nearly, 1)


def store(dims, mixed, synced, mixed_out, synced_out, mark, sems):
    n, _, el, _, nsub, late = dims
    p, core = lax.axis_index("dp"), lax.rem(lax.axis_index("expert"), 2)
    rows = synced.shape[1] // n
    own = (n - 1) * el * nsub - core * late

    def local_part(e):
        part = pl.ds(pl.multiple_of(p * rows, 16), rows)
        return pltpu.make_async_copy(synced.at[e, part], synced_out.at[e, part], sems.at[e])

    def arrived_part(i):
        offset, e, r = chunk_at(dims, i)
        part = rows_of(dims, rows, lax.rem(p + n - offset, n), r)
        return pltpu.make_async_copy(synced.at[e, part], synced_out.at[e, part], sems.at[el + i])

    out = pltpu.make_async_copy(mixed, mixed_out, sems.at[sems.shape[0] - 1])
    each(0, el, lambda e: local_part(e).start())
    each(0, own, lambda i: arrived_part(i).start())
    out.start()
    mark[...] = jnp.zeros_like(mark)
    each(0, el, lambda e: local_part(e).wait())
    each(0, own, lambda i: arrived_part(i).wait())
    out.wait()


def trailing(dims, trained, mark, tail, wide, narrow, wide_sem, send_sem, recv_sem):
    n, _, el, rc, nsub, late = dims
    p, me = lax.axis_index("dp"), lax.axis_index("expert")
    width = wide.shape[2]
    first = (n - 1) * el * nsub - late
    stop = lax.rem(me, 2) * late

    def load(i):
        offset, e, r = chunk_at(dims, first + i)
        cols = pl.ds(pl.multiple_of(lax.rem(p + offset, n) * width, 128), width)
        return pltpu.make_async_copy(
            trained.at[e, pl.ds(pl.multiple_of(r, 16), rc), cols], wide.at[i], wide_sem.at[i]
        )

    def copy(i):
        offset, _, _ = chunk_at(dims, first + i)
        return pltpu.make_async_remote_copy(
            src_ref=narrow.at[i],
            dst_ref=tail.at[i],
            send_sem=send_sem.at[i],
            recv_sem=recv_sem.at[i],
            device_id=(lax.rem(p + offset, n), me),
            device_id_type=MESH,
        )

    def send(i):
        load(i).wait()
        narrow[i] = wide[i].astype(jnp.bfloat16)
        copy(i).start()

    barrier = pltpu.get_barrier_semaphore()
    each(
        1, n,
        lambda o: pl.semaphore_signal(
            barrier, inc=1, device_id=(lax.rem(p + o, n), me), device_id_type=MESH
        ),
    )
    each(0, stop, lambda i: load(i).start())
    pl.semaphore_wait(barrier, n - 1)
    each(0, stop, send)
    each(0, stop, lambda i: copy(i).wait())


def settle(dims, tail, stored, synced_out, sems):
    n, _, el, _, nsub, late = dims
    p, core = lax.axis_index("dp"), lax.rem(lax.axis_index("expert"), 2)
    rows = synced_out.shape[1] // n
    first = (n - 1) * el * nsub - late

    def part(i):
        offset, e, r = chunk_at(dims, first + i)
        source = lax.rem(p + n - offset, n)
        return pltpu.make_async_copy(
            tail.at[i], synced_out.at[e, rows_of(dims, rows, source, r)], sems.at[i]
        )

    each(0, core * late, lambda i: part(i).start())
    each(0, core * late, lambda i: part(i).wait())


def local(tokens, routes, route_weight, gate_weight, up_weight, down_weight, trained_down):
    n, groups = lax.axis_size("dp"), lax.axis_size("expert")
    tok_rows, width = tokens.shape
    el, _, ff = gate_weight.shape
    rows = trained_down.shape[1]
    slots = el * CAP
    total = groups * slots
    share = total // n
    fits = [
        d for d in range(16, rows + 1, 16) if rows % d == 0 and d * width * 2 <= CHUNK_BYTES
    ]
    rc = fits[-1]
    nsub = rows // rc
    chunks = n * el * nsub
    remote = chunks - el * nsub
    late = round(remote * LATE)
    dims = (n, groups, el, rc, nsub, late)
    bf16, f32 = jnp.bfloat16, jnp.float32
    inside = pl.BlockSpec(memory_space=pltpu.VMEM)
    anywhere = pl.BlockSpec(memory_space=pl.ANY)
    dma = pltpu.SemaphoreType.DMA
    routes, route_weight = routes.T, route_weight.T

    def in_vmem(x):
        return pltpu.with_memory_space_constraint(x, pltpu.VMEM)

    mixed, synced = pl.pallas_call(
        functools.partial(fused, dims),
        out_shape=(
            pltpu.VMEM((tok_rows, width), bf16),
            pltpu.VMEM((el, n * rows, width), bf16),
        ),
        in_specs=[anywhere] * 7,
        out_specs=(inside, inside),
        scratch_shapes=[
            pltpu.VMEM(tokens.shape, bf16),
            pltpu.VMEM(routes.shape, jnp.int32),
            pltpu.VMEM(route_weight.shape, f32),
            pltpu.VMEM(gate_weight.shape, bf16),
            pltpu.VMEM(up_weight.shape, bf16),
            pltpu.VMEM(down_weight.shape, bf16),
            pltpu.VMEM((chunks, rc, width), f32),
            pltpu.VMEM((remote, rc, width), bf16),
            pltpu.VMEM((groups, slots, width), bf16),
            pltpu.VMEM((groups, slots, width), bf16),
            pltpu.VMEM((el, total // el, width), bf16),
            pltpu.VMEM((total, 2 * ff), f32),
            pltpu.VMEM((n, share, 2 * ff), bf16),
            pltpu.VMEM((n, share, 2 * ff), bf16),
            pltpu.VMEM((total, ff), bf16),
            pltpu.VMEM((groups, slots, width), bf16),
            pltpu.VMEM((groups, slots, width), bf16),
            dma((3,)),
            dma((3 * el,)),
            dma((chunks,)),
            dma((remote,)),
            dma((remote,)),
            dma((groups,)),
            dma((groups,)),
            dma((n,)),
            dma((n,)),
            dma((n,)),
            dma((n,)),
            dma((groups,)),
            dma((groups,)),
            pltpu.SemaphoreType.REGULAR,
            pltpu.SemaphoreType.REGULAR,
        ],
        compiler_params=pltpu.CompilerParams(
            collective_id=0, has_side_effects=True, vmem_limit_bytes=52 * 2**20
        ),
        cost_estimate=pl.CostEstimate(
            flops=6 * total * width * ff, bytes_accessed=2**28, transcendentals=0
        ),
    )(tokens, routes, route_weight, gate_weight, up_weight, down_weight, trained_down)
    mixed, stored, mark = pl.pallas_call(
        functools.partial(store, dims),
        out_shape=(
            jax.ShapeDtypeStruct((tok_rows, width), bf16),
            jax.ShapeDtypeStruct((el, n * rows, width), bf16),
            pltpu.VMEM((8, 128), f32),
        ),
        in_specs=[inside] * 2,
        out_specs=(anywhere, anywhere, inside),
        scratch_shapes=[dma((el + remote + 1,))],
        compiler_params=pltpu.CompilerParams(vmem_limit_bytes=2**20),
    )(in_vmem(mixed), in_vmem(synced))
    tail = pl.pallas_call(
        functools.partial(trailing, dims),
        out_shape=pltpu.VMEM((late, rc, width), bf16),
        in_specs=[anywhere] * 2,
        out_specs=inside,
        scratch_shapes=[
            pltpu.VMEM((late, rc, width), f32),
            pltpu.VMEM((late, rc, width), bf16),
            dma((late,)),
            dma((late,)),
            dma((late,)),
        ],
        compiler_params=pltpu.CompilerParams(
            collective_id=1, has_side_effects=True, vmem_limit_bytes=56 * 2**20
        ),
    )(trained_down, in_vmem(mark))
    synced = pl.pallas_call(
        functools.partial(settle, dims),
        out_shape=jax.ShapeDtypeStruct((el, n * rows, width), bf16),
        in_specs=[inside, anywhere],
        out_specs=anywhere,
        scratch_shapes=[dma((late,))],
        input_output_aliases={1: 0},
        compiler_params=pltpu.CompilerParams(vmem_limit_bytes=2**20),
    )(in_vmem(tail), stored)
    return mixed, synced


def solution(mesh):
    placed = (
        P("expert", "dp"),
        P("expert", None),
        P("expert", None),
        P("expert", "dp", None),
        P("expert", "dp", None),
        P("expert", None, "dp"),
        P("expert", "dp", None),
    )
    return jax.shard_map(
        local,
        mesh=mesh,
        in_specs=placed,
        out_specs=(P("expert", "dp"), P("expert", None, "dp")),
        check_vma=False,
    )
```

```python
import functools

import jax
import jax.numpy as jnp
from jax import lax
from jax.experimental import pallas as pl
from jax.experimental.pallas import tpu as pltpu
from jax.sharding import PartitionSpec as P

CAP = 4
CHUNK_BYTES = 200_000
FIRST = 2
EARLY = 5 / 16
MIDDLE = 1 / 16
LATE = 3 / 16
COVER = 4
TILT = 8
MESH = pl.DeviceIdType.MESH


def each(start, stop, body):
    def step(i, carry):
        body(i)
        return carry

    lax.fori_loop(start, stop, step, 0)


def chunk_at(dims, i):
    n, _, el, rc, nsub, _ = dims
    offset = lax.rem(lax.div(i, el * nsub) + 1, n)
    e = lax.rem(lax.div(i, nsub), el)
    return offset, e, lax.rem(i, nsub) * rc


def tilt_of(n, total):
    return total // TILT // 16 * 16 if n == 2 else 0


def rows_of(dims, rows, source, r):
    return pl.ds(pl.multiple_of(source * rows + r, 16), dims[3])


def fused(
    dims,
    tokens, routes, route_weight, gate_weight, up_weight, down_weight, trained,
    mixed, synced,
    tok_v, routes_v, weight_v, gate_v, up_v, down_v, wide, kept, narrow,
    outgoing, arrived, by_expert, partial, to_send, peers_part, to_tilt, peers_tilt, hidden,
    leaving, returned,
    small_sem, load_sem, wide_sem, kept_sem, sync_send, sync_recv,
    out_send, out_recv, part_send, part_recv, hid_send, hid_recv, ret_send, ret_recv,
    tilt_sem, entered, nearly,
):
    n, groups, el, rc, nsub, late = dims
    p, me = lax.axis_index("dp"), lax.axis_index("expert")
    core = lax.rem(me, 2)
    rows = trained.shape[1]
    tok_rows, width = tok_v.shape
    ff = gate_v.shape[2]
    slots = el * CAP
    total = groups * slots
    tilt = tilt_of(n, total)
    share = (total - tilt) // n
    tilted = pl.ds(n * share, tilt)
    per_expert = total // el
    per_peer = el * nsub
    remote = (n - 1) * per_peer
    early = round(remote * EARLY)
    middle = early + round(remote * MIDDLE)
    own = remote - core * late

    def peer(offset):
        return lax.rem(p + offset, n)

    def share_of(device):
        return pl.ds(pl.multiple_of(device * share, 16), share)

    def load_wide(i):
        offset, e, r = chunk_at(dims, i)
        cols = pl.ds(pl.multiple_of(peer(offset) * width, 128), width)
        return pltpu.make_async_copy(
            trained.at[e, pl.ds(pl.multiple_of(r, 16), rc), cols], wide.at[i], wide_sem.at[i]
        )

    def sync_copy(i):
        offset, e, r = chunk_at(dims, i)
        return pltpu.make_async_remote_copy(
            src_ref=narrow.at[i],
            dst_ref=synced.at[e, rows_of(dims, rows, p, r), :],
            send_sem=sync_send.at[i],
            recv_sem=sync_recv.at[i],
            device_id=(peer(offset), me),
            device_id_type=MESH,
        )

    def sync_arrival(i):
        offset, e, r = chunk_at(dims, i)
        source = lax.rem(p + n - offset, n)
        return pltpu.make_async_remote_copy(
            src_ref=narrow.at[i],
            dst_ref=synced.at[e, rows_of(dims, rows, source, r), :],
            send_sem=sync_send.at[i],
            recv_sem=sync_recv.at[i],
            device_id=(peer(offset), me),
            device_id_type=MESH,
        )

    load_kept = pltpu.make_async_copy(
        trained.at[:, :, pl.ds(pl.multiple_of(p * width, 128), width)], kept, kept_sem
    )

    def send_chunk(i):
        load_wide(i).wait()
        narrow[i] = wide[i].astype(jnp.bfloat16)
        sync_copy(i).start()

    def spread(source, target, send, recv, slot):
        return pltpu.make_async_remote_copy(
            src_ref=source.at[slot],
            dst_ref=target.at[me],
            send_sem=send,
            recv_sem=recv,
            device_id=(p, slot),
            device_id_type=MESH,
        )

    def spread_all(source, target, send, recv):
        each(
            1, groups,
            lambda o: spread(source, target, send, recv, lax.rem(me + o, groups)).start(),
        )

    def blocks(source, target, send, recv):
        some = pl.ds(0, groups - 1)
        return pltpu.make_async_remote_copy(
            src_ref=source.at[some],
            dst_ref=target.at[some],
            send_sem=send,
            recv_sem=recv,
            device_id=(p, lax.rem(me + 1, groups)),
            device_id_type=MESH,
        )

    def part_copy(o):
        return pltpu.make_async_remote_copy(
            src_ref=to_send.at[peer(o)],
            dst_ref=peers_part.at[o],
            send_sem=part_send.at[o],
            recv_sem=part_recv.at[o],
            device_id=(peer(o), me),
            device_id_type=MESH,
        )

    def hidden_copy(o, origin):
        return pltpu.make_async_remote_copy(
            src_ref=hidden.at[share_of(origin), :],
            dst_ref=hidden.at[share_of(origin), :],
            send_sem=hid_send.at[o],
            recv_sem=hid_recv.at[o],
            device_id=(peer(o), me),
            device_id_type=MESH,
        )

    def tilt_copy(source, target, k, device):
        return pltpu.make_async_remote_copy(
            src_ref=source,
            dst_ref=target,
            send_sem=tilt_sem.at[k],
            recv_sem=tilt_sem.at[k + 1],
            device_id=(device, me),
            device_id_type=MESH,
        )

    if tilt:
        tilt_part = tilt_copy(to_tilt, peers_tilt, 0, 1)
        tilt_hidden = tilt_copy(hidden.at[tilted, :], hidden.at[tilted, :], 2, 0)

    def activate(summed):
        gate, up = summed[:, :ff], summed[:, ff:]
        return (gate / (1.0 + jnp.exp(-gate)) * up).astype(jnp.bfloat16)

    smalls = [
        pltpu.make_async_copy(src, dst, small_sem.at[i])
        for i, (src, dst) in enumerate(
            ((routes, routes_v), (route_weight, weight_v), (tokens, tok_v))
        )
    ]

    def weights(k, src, dst):
        return lambda e: pltpu.make_async_copy(src.at[e], dst.at[e], load_sem.at[k * el + e])

    load_gate = weights(0, gate_weight, gate_v)
    load_up = weights(1, up_weight, up_v)
    load_down = weights(2, down_weight, down_v)

    barrier = pltpu.get_barrier_semaphore()

    def greet(device):
        pl.semaphore_signal(barrier, inc=1, device_id=device, device_id_type=MESH)

    each(0, FIRST, lambda i: load_wide(i).start())
    leader = me - core
    each(1, n, lambda o: greet((peer(o), me)))

    @pl.when(core == 0)
    def _():
        greet((p, me + 1))

    @pl.when(core == 1)
    def _():
        each(0, groups // 2, lambda j: greet((p, lax.rem(leader + 2 * j, groups))))

    @pl.when(core == 0)
    def _():
        each(1, groups // 2, lambda j: greet((p, lax.rem(leader + 2 * j, groups))))

    for copy in smalls:
        copy.start()
    each(FIRST, early, lambda i: load_wide(i).start())
    each(0, el, lambda e: load_gate(e).start())
    each(0, el, lambda e: load_up(e).start())
    each(early, own, lambda i: load_wide(i).start())
    each(0, el, lambda e: load_down(e).start())
    load_kept.start()
    pl.semaphore_wait(barrier, n - 1 + jnp.where(core == 0, groups - 1, 1))

    @pl.when(core == 0)
    def _():
        pl.semaphore_signal(entered, inc=1, device_id=(p, me + 1), device_id_type=MESH)

    each(0, FIRST, send_chunk)

    for copy in smalls:
        copy.wait()
    slot = lax.broadcasted_iota(jnp.int32, (total, tok_rows), 0)
    slot_expert = slot // CAP
    chosen = jnp.zeros((total, tok_rows), jnp.float32)
    scale = jnp.zeros((total, tok_rows), jnp.float32)
    for k in range(routes_v.shape[0]):
        hit = routes_v[k : k + 1, :] == slot_expert
        chosen = chosen + jnp.where(hit, 1.0, 0.0)
        scale = scale + jnp.where(hit, weight_v[k : k + 1, :], 0.0)
    row = lax.broadcasted_iota(jnp.int32, (tok_rows, tok_rows), 0)
    col = lax.broadcasted_iota(jnp.int32, (tok_rows, tok_rows), 1)
    before = jnp.where(row < col, 1.0, 0.0).astype(jnp.bfloat16)
    earlier = jnp.dot(chosen.astype(jnp.bfloat16), before, preferred_element_type=jnp.float32)
    placed = (chosen == 1.0) & (earlier == (slot % CAP).astype(jnp.float32))
    combine = jnp.where(placed, scale, 0.0).T
    dispatch = jnp.where(placed, 1.0, 0.0).astype(jnp.bfloat16)
    outgoing[...] = (
        jnp.dot(dispatch, tok_v[...], preferred_element_type=jnp.float32)
        .astype(jnp.bfloat16)
        .reshape(groups, slots, width)
    )
    arrived[me] = outgoing[me]

    @pl.when(core == 1)
    def _():
        pl.semaphore_wait(entered, 1)

    spread_all(outgoing, arrived, out_send, out_recv)
    each(FIRST, early, send_chunk)

    r = lax.broadcasted_iota(jnp.int32, (total, total), 0)
    c = lax.broadcasted_iota(jnp.int32, (total, total), 1)
    home = ((r // CAP) % groups) * slots + (r // per_expert) * CAP + r % CAP
    order = jnp.where(c == home, 1.0, 0.0)
    blocks(outgoing, arrived, out_send, out_recv).wait_recv()
    by_expert[...] = (
        jnp.dot(
            order.astype(jnp.bfloat16),
            arrived[...].reshape(total, width),
            preferred_element_type=jnp.float32,
        )
        .astype(jnp.bfloat16)
        .reshape(el, per_expert, width)
    )

    def project(e):
        load_gate(e).wait()
        load_up(e).wait()
        x = by_expert[e]
        at = pl.ds(pl.multiple_of(e * per_expert, 16), per_expert)
        partial[at, :ff] = jnp.dot(x, gate_v[e], preferred_element_type=jnp.float32)
        partial[at, ff:] = jnp.dot(x, up_v[e], preferred_element_type=jnp.float32)

    each(0, el, project)
    to_send[...] = partial[: n * share].reshape(n, share, 2 * ff).astype(jnp.bfloat16)
    each(1, n, lambda o: part_copy(o).start())
    if tilt:
        to_tilt[...] = partial[n * share :].astype(jnp.bfloat16)

        @pl.when(p == 0)
        def _():
            tilt_part.start()

    each(early, middle, send_chunk)

    each(1, n, lambda o: part_copy(o).wait_recv())

    def gather_part(o, acc):
        return acc + peers_part[o].astype(jnp.float32)

    summed = lax.fori_loop(1, n, gather_part, partial[share_of(p), :])
    hidden[share_of(p), :] = activate(summed)
    each(1, n, lambda o: hidden_copy(o, p).start())
    if tilt:

        @pl.when(p == 1)
        def _():
            tilt_part.wait_recv()
            hidden[tilted, :] = activate(partial[tilted, :] + peers_tilt[...].astype(jnp.float32))
            tilt_hidden.start()

    each(middle, own, send_chunk)
    each(1, n, lambda o: hidden_copy(o, lax.rem(p + n - o, n)).wait_recv())
    if tilt:

        @pl.when(p == 0)
        def _():
            tilt_hidden.wait_recv()


    def contract(e):
        load_down(e).wait()
        h = hidden[pl.ds(pl.multiple_of(e * per_expert, 16), per_expert), :]
        by_expert[e] = jnp.dot(h, down_v[e], preferred_element_type=jnp.float32).astype(
            jnp.bfloat16
        )

    each(0, el, contract)
    leaving[...] = (
        jnp.dot(
            order.T.astype(jnp.bfloat16),
            by_expert[...].reshape(total, width),
            preferred_element_type=jnp.float32,
        )
        .astype(jnp.bfloat16)
        .reshape(groups, slots, width)
    )
    returned[me] = leaving[me]
    spread_all(leaving, returned, ret_send, ret_recv)

    load_kept.wait()

    def keep(e):
        synced[e, pl.ds(pl.multiple_of(p * rows, 16), rows), :] = kept[e].astype(jnp.bfloat16)

    each(0, el, keep)
    blocks(leaving, returned, ret_send, ret_recv).wait_recv()
    answers = returned[...].reshape(total, width)
    high = combine.astype(jnp.bfloat16)
    rest = combine - high.astype(jnp.float32)
    mid = rest.astype(jnp.bfloat16)
    low = (rest - mid.astype(jnp.float32)).astype(jnp.bfloat16)
    mixed[...] = (
        jnp.dot(low, answers, preferred_element_type=jnp.float32)
        + jnp.dot(mid, answers, preferred_element_type=jnp.float32)
        + jnp.dot(high, answers, preferred_element_type=jnp.float32)
    ).astype(jnp.bfloat16)

    blocks(outgoing, arrived, out_send, out_recv).wait_send()
    blocks(leaving, returned, ret_send, ret_recv).wait_send()
    each(1, n, lambda o: part_copy(o).wait_send())
    each(1, n, lambda o: hidden_copy(o, p).wait_send())
    if tilt:

        @pl.when(p == 0)
        def _():
            tilt_part.wait_send()

        @pl.when(p == 1)
        def _():
            tilt_hidden.wait_send()


    def finish(i):
        sync_copy(i).wait_send()
        sync_arrival(i).wait_recv()

    each(0, own - COVER, finish)

    @pl.when(core == 0)
    def _():
        pl.semaphore_signal(nearly, inc=1, device_id=(p, me + 1), device_id_type=MESH)

    each(own - COVER, own, finish)

    @pl.when(core == 1)
    def _():
        pl.semaphore_wait(nearly, 1)


def store(dims, mixed, synced, mixed_out, synced_out, mark, sems):
    n, _, el, _, nsub, late = dims
    p, core = lax.axis_index("dp"), lax.rem(lax.axis_index("expert"), 2)
    rows = synced.shape[1] // n
    own = (n - 1) * el * nsub - core * late

    def local_part(e):
        part = pl.ds(pl.multiple_of(p * rows, 16), rows)
        return pltpu.make_async_copy(synced.at[e, part], synced_out.at[e, part], sems.at[e])

    def arrived_part(i):
        offset, e, r = chunk_at(dims, i)
        part = rows_of(dims, rows, lax.rem(p + n - offset, n), r)
        return pltpu.make_async_copy(synced.at[e, part], synced_out.at[e, part], sems.at[el + i])

    out = pltpu.make_async_copy(mixed, mixed_out, sems.at[sems.shape[0] - 1])
    each(0, el, lambda e: local_part(e).start())
    each(0, own, lambda i: arrived_part(i).start())
    out.start()
    mark[...] = jnp.zeros_like(mark)
    each(0, el, lambda e: local_part(e).wait())
    each(0, own, lambda i: arrived_part(i).wait())
    out.wait()


def trailing(dims, trained, mark, tail, wide, narrow, wide_sem, send_sem, recv_sem):
    n, _, el, rc, nsub, late = dims
    p, me = lax.axis_index("dp"), lax.axis_index("expert")
    width = wide.shape[2]
    first = (n - 1) * el * nsub - late

    def load(i):
        offset, e, r = chunk_at(dims, first + i)
        cols = pl.ds(pl.multiple_of(lax.rem(p + offset, n) * width, 128), width)
        return pltpu.make_async_copy(
            trained.at[e, pl.ds(pl.multiple_of(r, 16), rc), cols], wide.at[i], wide_sem.at[i]
        )

    def copy(i):
        offset, _, _ = chunk_at(dims, first + i)
        return pltpu.make_async_remote_copy(
            src_ref=narrow.at[i],
            dst_ref=tail.at[i],
            send_sem=send_sem.at[i],
            recv_sem=recv_sem.at[i],
            device_id=(lax.rem(p + offset, n), me),
            device_id_type=MESH,
        )

    def send(i):
        load(i).wait()
        narrow[i] = wide[i].astype(jnp.bfloat16)
        copy(i).start()

    @pl.when(lax.rem(me, 2) == 1)
    def _():
        barrier = pltpu.get_barrier_semaphore()
        each(
            1, n,
            lambda o: pl.semaphore_signal(
                barrier, inc=1, device_id=(lax.rem(p + o, n), me), device_id_type=MESH
            ),
        )
        each(0, late, lambda i: load(i).start())
        pl.semaphore_wait(barrier, n - 1)
        each(0, late, send)
        each(0, late, lambda i: copy(i).wait())


def settle(dims, tail, stored, synced_out, sems):
    n, _, el, _, nsub, late = dims
    p, core = lax.axis_index("dp"), lax.rem(lax.axis_index("expert"), 2)
    rows = synced_out.shape[1] // n
    first = (n - 1) * el * nsub - late

    def part(i):
        offset, e, r = chunk_at(dims, first + i)
        source = lax.rem(p + n - offset, n)
        return pltpu.make_async_copy(
            tail.at[i], synced_out.at[e, rows_of(dims, rows, source, r)], sems.at[i]
        )

    each(0, core * late, lambda i: part(i).start())
    each(0, core * late, lambda i: part(i).wait())


def local(tokens, routes, route_weight, gate_weight, up_weight, down_weight, trained_down):
    n, groups = lax.axis_size("dp"), lax.axis_size("expert")
    tok_rows, width = tokens.shape
    el, _, ff = gate_weight.shape
    rows = trained_down.shape[1]
    slots = el * CAP
    total = groups * slots
    tilt = tilt_of(n, total)
    share = (total - tilt) // n
    fits = [
        d for d in range(16, rows + 1, 16) if rows % d == 0 and d * width * 2 <= CHUNK_BYTES
    ]
    rc = fits[-1]
    nsub = rows // rc
    chunks = n * el * nsub
    remote = chunks - el * nsub
    late = round(remote * LATE)
    dims = (n, groups, el, rc, nsub, late)
    bf16, f32 = jnp.bfloat16, jnp.float32
    inside = pl.BlockSpec(memory_space=pltpu.VMEM)
    anywhere = pl.BlockSpec(memory_space=pl.ANY)
    dma = pltpu.SemaphoreType.DMA
    routes, route_weight = routes.T, route_weight.T

    def in_vmem(x):
        return pltpu.with_memory_space_constraint(x, pltpu.VMEM)

    mixed, synced = pl.pallas_call(
        functools.partial(fused, dims),
        out_shape=(
            pltpu.VMEM((tok_rows, width), bf16),
            pltpu.VMEM((el, n * rows, width), bf16),
        ),
        in_specs=[anywhere] * 7,
        out_specs=(inside, inside),
        scratch_shapes=[
            pltpu.VMEM(tokens.shape, bf16),
            pltpu.VMEM(routes.shape, jnp.int32),
            pltpu.VMEM(route_weight.shape, f32),
            pltpu.VMEM(gate_weight.shape, bf16),
            pltpu.VMEM(up_weight.shape, bf16),
            pltpu.VMEM(down_weight.shape, bf16),
            pltpu.VMEM((remote, rc, width), f32),
            pltpu.VMEM((el, rows, width), f32),
            pltpu.VMEM((remote, rc, width), bf16),
            pltpu.VMEM((groups, slots, width), bf16),
            pltpu.VMEM((groups, slots, width), bf16),
            pltpu.VMEM((el, total // el, width), bf16),
            pltpu.VMEM((total, 2 * ff), f32),
            pltpu.VMEM((n, share, 2 * ff), bf16),
            pltpu.VMEM((n, share, 2 * ff), bf16),
            pltpu.VMEM((max(tilt, 16), 2 * ff), bf16),
            pltpu.VMEM((max(tilt, 16), 2 * ff), bf16),
            pltpu.VMEM((total, ff), bf16),
            pltpu.VMEM((groups, slots, width), bf16),
            pltpu.VMEM((groups, slots, width), bf16),
            dma((3,)),
            dma((3 * el,)),
            dma((remote,)),
            dma(()),
            dma((remote,)),
            dma((remote,)),
            dma(()),
            dma(()),
            dma((n,)),
            dma((n,)),
            dma((n,)),
            dma((n,)),
            dma(()),
            dma(()),
            dma((4,)),
            pltpu.SemaphoreType.REGULAR,
            pltpu.SemaphoreType.REGULAR,
        ],
        compiler_params=pltpu.CompilerParams(
            collective_id=0, has_side_effects=True, vmem_limit_bytes=52 * 2**20
        ),
        cost_estimate=pl.CostEstimate(
            flops=6 * total * width * ff, bytes_accessed=2**28, transcendentals=0
        ),
    )(tokens, routes, route_weight, gate_weight, up_weight, down_weight, trained_down)
    mixed, stored, mark = pl.pallas_call(
        functools.partial(store, dims),
        out_shape=(
            jax.ShapeDtypeStruct((tok_rows, width), bf16),
            jax.ShapeDtypeStruct((el, n * rows, width), bf16),
            pltpu.VMEM((8, 128), f32),
        ),
        in_specs=[inside] * 2,
        out_specs=(anywhere, anywhere, inside),
        scratch_shapes=[dma((el + remote + 1,))],
        compiler_params=pltpu.CompilerParams(vmem_limit_bytes=2**20),
    )(in_vmem(mixed), in_vmem(synced))
    tail = pl.pallas_call(
        functools.partial(trailing, dims),
        out_shape=pltpu.VMEM((late, rc, width), bf16),
        in_specs=[anywhere] * 2,
        out_specs=inside,
        scratch_shapes=[
            pltpu.VMEM((late, rc, width), f32),
            pltpu.VMEM((late, rc, width), bf16),
            dma((late,)),
            dma((late,)),
            dma((late,)),
        ],
        compiler_params=pltpu.CompilerParams(
            collective_id=1, has_side_effects=True, vmem_limit_bytes=56 * 2**20
        ),
    )(trained_down, in_vmem(mark))
    synced = pl.pallas_call(
        functools.partial(settle, dims),
        out_shape=jax.ShapeDtypeStruct((el, n * rows, width), bf16),
        in_specs=[inside, anywhere],
        out_specs=anywhere,
        scratch_shapes=[dma((late,))],
        input_output_aliases={1: 0},
        compiler_params=pltpu.CompilerParams(vmem_limit_bytes=2**20),
    )(in_vmem(tail), stored)
    return mixed, synced


def solution(mesh):
    placed = (
        P("expert", "dp"),
        P("expert", None),
        P("expert", None),
        P("expert", "dp", None),
        P("expert", "dp", None),
        P("expert", None, "dp"),
        P("expert", "dp", None),
    )
    return jax.shard_map(
        local,
        mesh=mesh,
        in_specs=placed,
        out_specs=(P("expert", "dp"), P("expert", None, "dp")),
        check_vma=False,
    )
```

```python
import functools

import jax
import jax.numpy as jnp
from jax import lax
from jax.experimental import pallas as pl
from jax.experimental.pallas import tpu as pltpu
from jax.sharding import PartitionSpec as P

CAP = 4
CHUNK_BYTES = 200_000
FIRST = 2
EARLY = 5 / 16
MIDDLE = 1 / 16
LATE = 3 / 16
COVER = 4
TILT = 8
MESH = pl.DeviceIdType.MESH


def each(start, stop, body):
    def step(i, carry):
        body(i)
        return carry

    lax.fori_loop(start, stop, step, 0)


def chunk_at(dims, i):
    n, _, el, rc, nsub, _ = dims
    offset = lax.rem(lax.div(i, el * nsub) + 1, n)
    e = lax.rem(lax.div(i, nsub), el)
    return offset, e, lax.rem(i, nsub) * rc


def tilt_of(n, total):
    return total // TILT // 16 * 16 if n == 2 else 0


def rows_of(dims, rows, source, r):
    return pl.ds(pl.multiple_of(source * rows + r, 16), dims[3])


def fused(
    dims,
    tokens, routes, route_weight, gate_weight, up_weight, down_weight, trained,
    mixed, synced,
    tok_v, routes_v, weight_v, gate_v, up_v, down_v, wide, kept, narrow,
    outgoing, arrived, by_expert, partial, to_send, peers_part, to_tilt, peers_tilt, hidden,
    leaving, returned,
    small_sem, load_sem, wide_sem, kept_sem, sync_send, sync_recv,
    out_send, out_recv, part_send, part_recv, hid_send, hid_recv, ret_send, ret_recv,
    tilt_sem, entered, nearly,
):
    n, groups, el, rc, nsub, late = dims
    p, me = lax.axis_index("dp"), lax.axis_index("expert")
    core = lax.rem(me, 2)
    rows = trained.shape[1]
    tok_rows, width = tok_v.shape
    ff = gate_v.shape[2]
    slots = el * CAP
    total = groups * slots
    tilt = tilt_of(n, total)
    share = (total - tilt) // n
    tilted = pl.ds(n * share, tilt)
    per_expert = total // el
    per_peer = el * nsub
    remote = (n - 1) * per_peer
    early = round(remote * EARLY)
    middle = early + round(remote * MIDDLE)
    own = remote - core * late

    def peer(offset):
        return lax.rem(p + offset, n)

    def share_of(device):
        return pl.ds(pl.multiple_of(device * share, 16), share)

    def load_wide(i):
        offset, e, r = chunk_at(dims, i)
        cols = pl.ds(pl.multiple_of(peer(offset) * width, 128), width)
        return pltpu.make_async_copy(
            trained.at[e, pl.ds(pl.multiple_of(r, 16), rc), cols], wide.at[i], wide_sem.at[i]
        )

    def sync_copy(i):
        offset, e, r = chunk_at(dims, i)
        return pltpu.make_async_remote_copy(
            src_ref=narrow.at[i],
            dst_ref=synced.at[e, rows_of(dims, rows, p, r), :],
            send_sem=sync_send.at[i],
            recv_sem=sync_recv.at[i],
            device_id=(peer(offset), me),
            device_id_type=MESH,
        )

    def sync_arrival(i):
        offset, e, r = chunk_at(dims, i)
        source = lax.rem(p + n - offset, n)
        return pltpu.make_async_remote_copy(
            src_ref=narrow.at[i],
            dst_ref=synced.at[e, rows_of(dims, rows, source, r), :],
            send_sem=sync_send.at[i],
            recv_sem=sync_recv.at[i],
            device_id=(peer(offset), me),
            device_id_type=MESH,
        )

    load_kept = pltpu.make_async_copy(
        trained.at[:, :, pl.ds(pl.multiple_of(p * width, 128), width)], kept, kept_sem
    )

    def send_chunk(i):
        load_wide(i).wait()
        narrow[i] = wide[i].astype(jnp.bfloat16)
        sync_copy(i).start()

    def spread(source, target, send, recv, slot):
        return pltpu.make_async_remote_copy(
            src_ref=source.at[slot],
            dst_ref=target.at[me],
            send_sem=send,
            recv_sem=recv,
            device_id=(p, slot),
            device_id_type=MESH,
        )

    def spread_all(source, target, send, recv):
        each(
            1, groups,
            lambda o: spread(source, target, send, recv, lax.rem(me + o, groups)).start(),
        )

    def blocks(source, target, send, recv):
        some = pl.ds(0, groups - 1)
        return pltpu.make_async_remote_copy(
            src_ref=source.at[some],
            dst_ref=target.at[some],
            send_sem=send,
            recv_sem=recv,
            device_id=(p, lax.rem(me + 1, groups)),
            device_id_type=MESH,
        )

    def part_copy(o):
        return pltpu.make_async_remote_copy(
            src_ref=to_send.at[peer(o)],
            dst_ref=peers_part.at[o],
            send_sem=part_send.at[o],
            recv_sem=part_recv.at[o],
            device_id=(peer(o), me),
            device_id_type=MESH,
        )

    def hidden_copy(o, origin):
        return pltpu.make_async_remote_copy(
            src_ref=hidden.at[share_of(origin), :],
            dst_ref=hidden.at[share_of(origin), :],
            send_sem=hid_send.at[o],
            recv_sem=hid_recv.at[o],
            device_id=(peer(o), me),
            device_id_type=MESH,
        )

    def tilt_copy(source, target, k, device):
        return pltpu.make_async_remote_copy(
            src_ref=source,
            dst_ref=target,
            send_sem=tilt_sem.at[k],
            recv_sem=tilt_sem.at[k + 1],
            device_id=(device, me),
            device_id_type=MESH,
        )

    if tilt:
        tilt_part = tilt_copy(to_tilt, peers_tilt, 0, 1)
        tilt_hidden = tilt_copy(hidden.at[tilted, :], hidden.at[tilted, :], 2, 0)

    def activate(summed):
        gate, up = summed[:, :ff], summed[:, ff:]
        return (gate / (1.0 + jnp.exp(-gate)) * up).astype(jnp.bfloat16)

    smalls = [
        pltpu.make_async_copy(src, dst, small_sem.at[i])
        for i, (src, dst) in enumerate(
            ((routes, routes_v), (route_weight, weight_v), (tokens, tok_v))
        )
    ]

    def weights(k, src, dst):
        return lambda e: pltpu.make_async_copy(src.at[e], dst.at[e], load_sem.at[k * el + e])

    load_gate = weights(0, gate_weight, gate_v)
    load_up = weights(1, up_weight, up_v)
    load_down = weights(2, down_weight, down_v)

    barrier = pltpu.get_barrier_semaphore()

    def greet(device):
        pl.semaphore_signal(barrier, inc=1, device_id=device, device_id_type=MESH)

    each(0, FIRST, lambda i: load_wide(i).start())
    leader = me - core
    each(1, n, lambda o: greet((peer(o), me)))

    @pl.when(core == 0)
    def _():
        greet((p, me + 1))

    @pl.when(core == 1)
    def _():
        each(0, groups // 2, lambda j: greet((p, lax.rem(leader + 2 * j, groups))))

    @pl.when(core == 0)
    def _():
        each(1, groups // 2, lambda j: greet((p, lax.rem(leader + 2 * j, groups))))

    for copy in smalls:
        copy.start()
    each(FIRST, early, lambda i: load_wide(i).start())
    each(0, el, lambda e: load_gate(e).start())
    each(0, el, lambda e: load_up(e).start())
    each(early, own, lambda i: load_wide(i).start())
    each(0, el, lambda e: load_down(e).start())
    load_kept.start()
    pl.semaphore_wait(barrier, n - 1 + jnp.where(core == 0, groups - 1, 1))

    @pl.when(core == 0)
    def _():
        pl.semaphore_signal(entered, inc=1, device_id=(p, me + 1), device_id_type=MESH)

    each(0, early, send_chunk)

    for copy in smalls:
        copy.wait()
    slot = lax.broadcasted_iota(jnp.int32, (total, tok_rows), 0)
    slot_expert = slot // CAP
    chosen = jnp.zeros((total, tok_rows), jnp.float32)
    scale = jnp.zeros((total, tok_rows), jnp.float32)
    for k in range(routes_v.shape[0]):
        hit = routes_v[k : k + 1, :] == slot_expert
        chosen = chosen + jnp.where(hit, 1.0, 0.0)
        scale = scale + jnp.where(hit, weight_v[k : k + 1, :], 0.0)
    row = lax.broadcasted_iota(jnp.int32, (tok_rows, tok_rows), 0)
    col = lax.broadcasted_iota(jnp.int32, (tok_rows, tok_rows), 1)
    before = jnp.where(row < col, 1.0, 0.0).astype(jnp.bfloat16)
    earlier = jnp.dot(chosen.astype(jnp.bfloat16), before, preferred_element_type=jnp.float32)
    placed = (chosen == 1.0) & (earlier == (slot % CAP).astype(jnp.float32))
    combine = jnp.where(placed, scale, 0.0).T
    dispatch = jnp.where(placed, 1.0, 0.0).astype(jnp.bfloat16)
    outgoing[...] = (
        jnp.dot(dispatch, tok_v[...], preferred_element_type=jnp.float32)
        .astype(jnp.bfloat16)
        .reshape(groups, slots, width)
    )
    arrived[me] = outgoing[me]

    @pl.when(core == 1)
    def _():
        pl.semaphore_wait(entered, 1)

    spread_all(outgoing, arrived, out_send, out_recv)

    r = lax.broadcasted_iota(jnp.int32, (total, total), 0)
    c = lax.broadcasted_iota(jnp.int32, (total, total), 1)
    home = ((r // CAP) % groups) * slots + (r // per_expert) * CAP + r % CAP
    order = jnp.where(c == home, 1.0, 0.0)
    blocks(outgoing, arrived, out_send, out_recv).wait_recv()
    by_expert[...] = (
        jnp.dot(
            order.astype(jnp.bfloat16),
            arrived[...].reshape(total, width),
            preferred_element_type=jnp.float32,
        )
        .astype(jnp.bfloat16)
        .reshape(el, per_expert, width)
    )

    def project(e):
        load_gate(e).wait()
        load_up(e).wait()
        x = by_expert[e]
        at = pl.ds(pl.multiple_of(e * per_expert, 16), per_expert)
        partial[at, :ff] = jnp.dot(x, gate_v[e], preferred_element_type=jnp.float32)
        partial[at, ff:] = jnp.dot(x, up_v[e], preferred_element_type=jnp.float32)

    each(0, el, project)
    to_send[...] = partial[: n * share].reshape(n, share, 2 * ff).astype(jnp.bfloat16)
    each(1, n, lambda o: part_copy(o).start())
    if tilt:
        to_tilt[...] = partial[n * share :].astype(jnp.bfloat16)

        @pl.when(p == 0)
        def _():
            tilt_part.start()

    each(early, middle, send_chunk)

    each(1, n, lambda o: part_copy(o).wait_recv())

    def gather_part(o, acc):
        return acc + peers_part[o].astype(jnp.float32)

    summed = lax.fori_loop(1, n, gather_part, partial[share_of(p), :])
    hidden[share_of(p), :] = activate(summed)
    each(1, n, lambda o: hidden_copy(o, p).start())
    if tilt:

        @pl.when(p == 1)
        def _():
            tilt_part.wait_recv()
            hidden[tilted, :] = activate(partial[tilted, :] + peers_tilt[...].astype(jnp.float32))
            tilt_hidden.start()

    each(middle, own, send_chunk)
    each(1, n, lambda o: hidden_copy(o, lax.rem(p + n - o, n)).wait_recv())
    if tilt:

        @pl.when(p == 0)
        def _():
            tilt_hidden.wait_recv()


    def contract(e):
        load_down(e).wait()
        h = hidden[pl.ds(pl.multiple_of(e * per_expert, 16), per_expert), :]
        by_expert[e] = jnp.dot(h, down_v[e], preferred_element_type=jnp.float32).astype(
            jnp.bfloat16
        )

    each(0, el, contract)
    leaving[...] = (
        jnp.dot(
            order.T.astype(jnp.bfloat16),
            by_expert[...].reshape(total, width),
            preferred_element_type=jnp.float32,
        )
        .astype(jnp.bfloat16)
        .reshape(groups, slots, width)
    )
    returned[me] = leaving[me]
    spread_all(leaving, returned, ret_send, ret_recv)

    load_kept.wait()

    def keep(e):
        synced[e, pl.ds(pl.multiple_of(p * rows, 16), rows), :] = kept[e].astype(jnp.bfloat16)

    each(0, el, keep)
    blocks(leaving, returned, ret_send, ret_recv).wait_recv()
    answers = returned[...].reshape(total, width)
    high = combine.astype(jnp.bfloat16)
    rest = combine - high.astype(jnp.float32)
    mid = rest.astype(jnp.bfloat16)
    low = (rest - mid.astype(jnp.float32)).astype(jnp.bfloat16)
    mixed[...] = (
        jnp.dot(low, answers, preferred_element_type=jnp.float32)
        + jnp.dot(mid, answers, preferred_element_type=jnp.float32)
        + jnp.dot(high, answers, preferred_element_type=jnp.float32)
    ).astype(jnp.bfloat16)

    blocks(outgoing, arrived, out_send, out_recv).wait_send()
    blocks(leaving, returned, ret_send, ret_recv).wait_send()
    each(1, n, lambda o: part_copy(o).wait_send())
    each(1, n, lambda o: hidden_copy(o, p).wait_send())
    if tilt:

        @pl.when(p == 0)
        def _():
            tilt_part.wait_send()

        @pl.when(p == 1)
        def _():
            tilt_hidden.wait_send()


    def finish(i):
        sync_copy(i).wait_send()
        sync_arrival(i).wait_recv()

    each(0, own - COVER, finish)

    @pl.when(core == 0)
    def _():
        pl.semaphore_signal(nearly, inc=1, device_id=(p, me + 1), device_id_type=MESH)

    each(own - COVER, own, finish)

    @pl.when(core == 1)
    def _():
        pl.semaphore_wait(nearly, 1)


def store(dims, mixed, synced, mixed_out, synced_out, mark, sems):
    n, _, el, _, nsub, late = dims
    p, core = lax.axis_index("dp"), lax.rem(lax.axis_index("expert"), 2)
    rows = synced.shape[1] // n
    own = (n - 1) * el * nsub - core * late

    def local_part(e):
        part = pl.ds(pl.multiple_of(p * rows, 16), rows)
        return pltpu.make_async_copy(synced.at[e, part], synced_out.at[e, part], sems.at[e])

    def arrived_part(i):
        offset, e, r = chunk_at(dims, i)
        part = rows_of(dims, rows, lax.rem(p + n - offset, n), r)
        return pltpu.make_async_copy(synced.at[e, part], synced_out.at[e, part], sems.at[el + i])

    out = pltpu.make_async_copy(mixed, mixed_out, sems.at[sems.shape[0] - 1])
    each(0, el, lambda e: local_part(e).start())
    each(0, own, lambda i: arrived_part(i).start())
    out.start()
    mark[...] = jnp.zeros_like(mark)
    each(0, el, lambda e: local_part(e).wait())
    each(0, own, lambda i: arrived_part(i).wait())
    out.wait()


def trailing(dims, trained, mark, tail, wide, narrow, wide_sem, send_sem, recv_sem):
    n, _, el, rc, nsub, late = dims
    p, me = lax.axis_index("dp"), lax.axis_index("expert")
    width = wide.shape[2]
    first = (n - 1) * el * nsub - late

    def load(i):
        offset, e, r = chunk_at(dims, first + i)
        cols = pl.ds(pl.multiple_of(lax.rem(p + offset, n) * width, 128), width)
        return pltpu.make_async_copy(
            trained.at[e, pl.ds(pl.multiple_of(r, 16), rc), cols], wide.at[i], wide_sem.at[i]
        )

    def copy(i):
        offset, _, _ = chunk_at(dims, first + i)
        return pltpu.make_async_remote_copy(
            src_ref=narrow.at[i],
            dst_ref=tail.at[i],
            send_sem=send_sem,
            recv_sem=recv_sem,
            device_id=(lax.rem(p + offset, n), me),
            device_id_type=MESH,
        )

    def send(i):
        load(i).wait()
        narrow[i] = wide[i].astype(jnp.bfloat16)
        copy(i).start()

    @pl.when(lax.rem(me, 2) == 1)
    def _():
        barrier = pltpu.get_barrier_semaphore()
        each(
            1, n,
            lambda o: pl.semaphore_signal(
                barrier, inc=1, device_id=(lax.rem(p + o, n), me), device_id_type=MESH
            ),
        )
        each(0, late, lambda i: load(i).start())
        pl.semaphore_wait(barrier, n - 1)
        each(0, late, send)
        pltpu.make_async_remote_copy(
            src_ref=narrow,
            dst_ref=tail,
            send_sem=send_sem,
            recv_sem=recv_sem,
            device_id=(lax.rem(p + 1, n), me),
            device_id_type=MESH,
        ).wait()


def settle(dims, tail, stored, synced_out, sems):
    n, _, el, _, nsub, late = dims
    p, core = lax.axis_index("dp"), lax.rem(lax.axis_index("expert"), 2)
    rows = synced_out.shape[1] // n
    first = (n - 1) * el * nsub - late

    def part(i):
        offset, e, r = chunk_at(dims, first + i)
        source = lax.rem(p + n - offset, n)
        return pltpu.make_async_copy(
            tail.at[i], synced_out.at[e, rows_of(dims, rows, source, r)], sems.at[i]
        )

    each(0, core * late, lambda i: part(i).start())
    each(0, core * late, lambda i: part(i).wait())


def local(tokens, routes, route_weight, gate_weight, up_weight, down_weight, trained_down):
    n, groups = lax.axis_size("dp"), lax.axis_size("expert")
    tok_rows, width = tokens.shape
    el, _, ff = gate_weight.shape
    rows = trained_down.shape[1]
    slots = el * CAP
    total = groups * slots
    tilt = tilt_of(n, total)
    share = (total - tilt) // n
    fits = [
        d for d in range(16, rows + 1, 16) if rows % d == 0 and d * width * 2 <= CHUNK_BYTES
    ]
    rc = fits[-1]
    nsub = rows // rc
    chunks = n * el * nsub
    remote = chunks - el * nsub
    late = round(remote * LATE)
    dims = (n, groups, el, rc, nsub, late)
    bf16, f32 = jnp.bfloat16, jnp.float32
    inside = pl.BlockSpec(memory_space=pltpu.VMEM)
    anywhere = pl.BlockSpec(memory_space=pl.ANY)
    dma = pltpu.SemaphoreType.DMA
    routes, route_weight = routes.T, route_weight.T

    def in_vmem(x):
        return pltpu.with_memory_space_constraint(x, pltpu.VMEM)

    mixed, synced = pl.pallas_call(
        functools.partial(fused, dims),
        out_shape=(
            pltpu.VMEM((tok_rows, width), bf16),
            pltpu.VMEM((el, n * rows, width), bf16),
        ),
        in_specs=[anywhere] * 7,
        out_specs=(inside, inside),
        scratch_shapes=[
            pltpu.VMEM(tokens.shape, bf16),
            pltpu.VMEM(routes.shape, jnp.int32),
            pltpu.VMEM(route_weight.shape, f32),
            pltpu.VMEM(gate_weight.shape, bf16),
            pltpu.VMEM(up_weight.shape, bf16),
            pltpu.VMEM(down_weight.shape, bf16),
            pltpu.VMEM((remote, rc, width), f32),
            pltpu.VMEM((el, rows, width), f32),
            pltpu.VMEM((remote, rc, width), bf16),
            pltpu.VMEM((groups, slots, width), bf16),
            pltpu.VMEM((groups, slots, width), bf16),
            pltpu.VMEM((el, total // el, width), bf16),
            pltpu.VMEM((total, 2 * ff), f32),
            pltpu.VMEM((n, share, 2 * ff), bf16),
            pltpu.VMEM((n, share, 2 * ff), bf16),
            pltpu.VMEM((max(tilt, 16), 2 * ff), bf16),
            pltpu.VMEM((max(tilt, 16), 2 * ff), bf16),
            pltpu.VMEM((total, ff), bf16),
            pltpu.VMEM((groups, slots, width), bf16),
            pltpu.VMEM((groups, slots, width), bf16),
            dma((3,)),
            dma((3 * el,)),
            dma((remote,)),
            dma(()),
            dma((remote,)),
            dma((remote,)),
            dma(()),
            dma(()),
            dma((n,)),
            dma((n,)),
            dma((n,)),
            dma((n,)),
            dma(()),
            dma(()),
            dma((4,)),
            pltpu.SemaphoreType.REGULAR,
            pltpu.SemaphoreType.REGULAR,
        ],
        compiler_params=pltpu.CompilerParams(
            collective_id=0, has_side_effects=True, vmem_limit_bytes=52 * 2**20
        ),
        cost_estimate=pl.CostEstimate(
            flops=6 * total * width * ff, bytes_accessed=2**28, transcendentals=0
        ),
    )(tokens, routes, route_weight, gate_weight, up_weight, down_weight, trained_down)
    mixed, stored, mark = pl.pallas_call(
        functools.partial(store, dims),
        out_shape=(
            jax.ShapeDtypeStruct((tok_rows, width), bf16),
            jax.ShapeDtypeStruct((el, n * rows, width), bf16),
            pltpu.VMEM((8, 128), f32),
        ),
        in_specs=[inside] * 2,
        out_specs=(anywhere, anywhere, inside),
        scratch_shapes=[dma((el + remote + 1,))],
        compiler_params=pltpu.CompilerParams(vmem_limit_bytes=2**20),
    )(in_vmem(mixed), in_vmem(synced))
    tail = pl.pallas_call(
        functools.partial(trailing, dims),
        out_shape=pltpu.VMEM((late, rc, width), bf16),
        in_specs=[anywhere] * 2,
        out_specs=inside,
        scratch_shapes=[
            pltpu.VMEM((late, rc, width), f32),
            pltpu.VMEM((late, rc, width), bf16),
            dma((late,)),
            dma(()),
            dma(()),
        ],
        compiler_params=pltpu.CompilerParams(
            collective_id=1, has_side_effects=True, vmem_limit_bytes=56 * 2**20
        ),
    )(trained_down, in_vmem(mark))
    synced = pl.pallas_call(
        functools.partial(settle, dims),
        out_shape=jax.ShapeDtypeStruct((el, n * rows, width), bf16),
        in_specs=[inside, anywhere],
        out_specs=anywhere,
        scratch_shapes=[dma((late,))],
        input_output_aliases={1: 0},
        compiler_params=pltpu.CompilerParams(vmem_limit_bytes=2**20),
    )(in_vmem(tail), stored)
    return mixed, synced


def solution(mesh):
    placed = (
        P("expert", "dp"),
        P("expert", None),
        P("expert", None),
        P("expert", "dp", None),
        P("expert", "dp", None),
        P("expert", None, "dp"),
        P("expert", "dp", None),
    )
    return jax.shard_map(
        local,
        mesh=mesh,
        in_specs=placed,
        out_specs=(P("expert", "dp"), P("expert", None, "dp")),
        check_vma=False,
    )
```

```python
import functools

import jax
import jax.numpy as jnp
from jax import lax
from jax.experimental import pallas as pl
from jax.experimental.pallas import tpu as pltpu
from jax.sharding import PartitionSpec as P

CAP = 4
CHUNK_BYTES = 200_000
FIRST = 1
EARLY = 5 / 16
MIDDLE = 1 / 16
LATE = 3 / 16
COVER = 4
TILT = 8
MESH = pl.DeviceIdType.MESH


def each(start, stop, body):
    def step(i, carry):
        body(i)
        return carry

    lax.fori_loop(start, stop, step, 0)


def chunk_at(dims, i):
    n, _, el, rc, nsub, _ = dims
    offset = lax.rem(lax.div(i, el * nsub) + 1, n)
    e = lax.rem(lax.div(i, nsub), el)
    return offset, e, lax.rem(i, nsub) * rc


def tilt_of(n, total):
    return total // TILT // 16 * 16 if n == 2 else 0


def rows_of(dims, rows, source, r):
    return pl.ds(pl.multiple_of(source * rows + r, 16), dims[3])


def fused(
    dims,
    tokens, routes, route_weight, gate_weight, up_weight, down_weight, trained,
    mixed, synced,
    tok_v, routes_v, weight_v, gate_v, up_v, down_v, wide, kept, narrow,
    outgoing, arrived, by_expert, partial, to_send, peers_part, to_tilt, peers_tilt, hidden,
    leaving, returned,
    small_sem, load_sem, wide_sem, kept_sem, sync_send, sync_recv,
    out_send, out_recv, part_send, part_recv, hid_send, hid_recv, ret_send, ret_recv,
    tilt_sem, entered, nearly,
):
    n, groups, el, rc, nsub, late = dims
    p, me = lax.axis_index("dp"), lax.axis_index("expert")
    core = lax.rem(me, 2)
    rows = trained.shape[1]
    tok_rows, width = tok_v.shape
    ff = gate_v.shape[2]
    slots = el * CAP
    total = groups * slots
    tilt = tilt_of(n, total)
    share = (total - tilt) // n
    tilted = pl.ds(n * share, tilt)
    per_expert = total // el
    per_peer = el * nsub
    remote = (n - 1) * per_peer
    early = round(remote * EARLY)
    middle = early + round(remote * MIDDLE)
    own = remote - core * late
    cover = min(COVER, remote - late)

    def peer(offset):
        return lax.rem(p + offset, n)

    def share_of(device):
        return pl.ds(pl.multiple_of(device * share, 16), share)

    def load_wide(i):
        offset, e, r = chunk_at(dims, i)
        cols = pl.ds(pl.multiple_of(peer(offset) * width, 128), width)
        return pltpu.make_async_copy(
            trained.at[e, pl.ds(pl.multiple_of(r, 16), rc), cols], wide.at[i], wide_sem.at[i]
        )

    def sync_copy(i):
        offset, e, r = chunk_at(dims, i)
        return pltpu.make_async_remote_copy(
            src_ref=narrow.at[i],
            dst_ref=synced.at[e, rows_of(dims, rows, p, r), :],
            send_sem=sync_send.at[i],
            recv_sem=sync_recv.at[i],
            device_id=(peer(offset), me),
            device_id_type=MESH,
        )

    def sync_arrival(i):
        offset, e, r = chunk_at(dims, i)
        source = lax.rem(p + n - offset, n)
        return pltpu.make_async_remote_copy(
            src_ref=narrow.at[i],
            dst_ref=synced.at[e, rows_of(dims, rows, source, r), :],
            send_sem=sync_send.at[i],
            recv_sem=sync_recv.at[i],
            device_id=(peer(offset), me),
            device_id_type=MESH,
        )

    load_kept = pltpu.make_async_copy(
        trained.at[:, :, pl.ds(pl.multiple_of(p * width, 128), width)], kept, kept_sem
    )

    def send_chunk(i):
        load_wide(i).wait()
        narrow[i] = wide[i].astype(jnp.bfloat16)
        sync_copy(i).start()

    def spread(source, target, send, recv, slot):
        return pltpu.make_async_remote_copy(
            src_ref=source.at[slot],
            dst_ref=target.at[me],
            send_sem=send,
            recv_sem=recv,
            device_id=(p, slot),
            device_id_type=MESH,
        )

    def spread_all(source, target, send, recv):
        each(
            1, groups,
            lambda o: spread(source, target, send, recv, lax.rem(me + o, groups)).start(),
        )

    def blocks(source, target, send, recv):
        some = pl.ds(0, groups - 1)
        return pltpu.make_async_remote_copy(
            src_ref=source.at[some],
            dst_ref=target.at[some],
            send_sem=send,
            recv_sem=recv,
            device_id=(p, lax.rem(me + 1, groups)),
            device_id_type=MESH,
        )

    def part_copy(o):
        return pltpu.make_async_remote_copy(
            src_ref=to_send.at[peer(o)],
            dst_ref=peers_part.at[o],
            send_sem=part_send.at[o],
            recv_sem=part_recv.at[o],
            device_id=(peer(o), me),
            device_id_type=MESH,
        )

    def hidden_copy(o, origin):
        return pltpu.make_async_remote_copy(
            src_ref=hidden.at[share_of(origin), :],
            dst_ref=hidden.at[share_of(origin), :],
            send_sem=hid_send.at[o],
            recv_sem=hid_recv.at[o],
            device_id=(peer(o), me),
            device_id_type=MESH,
        )

    def tilt_copy(source, target, k, device):
        return pltpu.make_async_remote_copy(
            src_ref=source,
            dst_ref=target,
            send_sem=tilt_sem.at[k],
            recv_sem=tilt_sem.at[k + 1],
            device_id=(device, me),
            device_id_type=MESH,
        )

    if tilt:
        tilt_part = tilt_copy(to_tilt, peers_tilt, 0, 1)
        tilt_hidden = tilt_copy(hidden.at[tilted, :], hidden.at[tilted, :], 2, 0)

    def activate(summed):
        gate, up = summed[:, :ff], summed[:, ff:]
        return (gate / (1.0 + jnp.exp(-gate)) * up).astype(jnp.bfloat16)

    smalls = [
        pltpu.make_async_copy(src, dst, small_sem.at[i])
        for i, (src, dst) in enumerate(
            ((routes, routes_v), (route_weight, weight_v), (tokens, tok_v))
        )
    ]

    def weights(k, src, dst):
        return lambda e: pltpu.make_async_copy(src.at[e], dst.at[e], load_sem.at[k * el + e])

    load_gate = weights(0, gate_weight, gate_v)
    load_up = weights(1, up_weight, up_v)
    load_down = weights(2, down_weight, down_v)

    barrier = pltpu.get_barrier_semaphore()

    def greet(device):
        pl.semaphore_signal(barrier, inc=1, device_id=device, device_id_type=MESH)

    each(0, FIRST, lambda i: load_wide(i).start())
    leader = me - core
    each(1, n, lambda o: greet((peer(o), me)))

    @pl.when(core == 0)
    def _():
        greet((p, me + 1))

    @pl.when(core == 1)
    def _():
        each(0, groups // 2, lambda j: greet((p, lax.rem(leader + 2 * j, groups))))

    @pl.when(core == 0)
    def _():
        each(1, groups // 2, lambda j: greet((p, lax.rem(leader + 2 * j, groups))))

    for copy in smalls:
        copy.start()
    each(FIRST, early, lambda i: load_wide(i).start())
    each(0, el, lambda e: load_gate(e).start())
    each(0, el, lambda e: load_up(e).start())
    each(early, own, lambda i: load_wide(i).start())
    each(0, el, lambda e: load_down(e).start())
    load_kept.start()
    pl.semaphore_wait(barrier, n - 1 + jnp.where(core == 0, groups - 1, 1))

    @pl.when(core == 0)
    def _():
        pl.semaphore_signal(entered, inc=1, device_id=(p, me + 1), device_id_type=MESH)

    each(0, early, send_chunk)

    for copy in smalls:
        copy.wait()
    slot = lax.broadcasted_iota(jnp.int32, (total, tok_rows), 0)
    slot_expert = slot // CAP
    chosen = jnp.zeros((total, tok_rows), jnp.float32)
    scale = jnp.zeros((total, tok_rows), jnp.float32)
    for k in range(routes_v.shape[0]):
        hit = routes_v[k : k + 1, :] == slot_expert
        chosen = chosen + jnp.where(hit, 1.0, 0.0)
        scale = scale + jnp.where(hit, weight_v[k : k + 1, :], 0.0)
    row = lax.broadcasted_iota(jnp.int32, (tok_rows, tok_rows), 0)
    col = lax.broadcasted_iota(jnp.int32, (tok_rows, tok_rows), 1)
    before = jnp.where(row < col, 1.0, 0.0).astype(jnp.bfloat16)
    earlier = jnp.dot(chosen.astype(jnp.bfloat16), before, preferred_element_type=jnp.float32)
    placed = (chosen == 1.0) & (earlier == (slot % CAP).astype(jnp.float32))
    combine = jnp.where(placed, scale, 0.0).T
    dispatch = jnp.where(placed, 1.0, 0.0).astype(jnp.bfloat16)
    outgoing[...] = (
        jnp.dot(dispatch, tok_v[...], preferred_element_type=jnp.float32)
        .astype(jnp.bfloat16)
        .reshape(groups, slots, width)
    )
    arrived[me] = outgoing[me]

    @pl.when(core == 1)
    def _():
        pl.semaphore_wait(entered, 1)

    spread_all(outgoing, arrived, out_send, out_recv)

    r = lax.broadcasted_iota(jnp.int32, (total, total), 0)
    c = lax.broadcasted_iota(jnp.int32, (total, total), 1)
    home = ((r // CAP) % groups) * slots + (r // per_expert) * CAP + r % CAP
    order = jnp.where(c == home, 1.0, 0.0)
    blocks(outgoing, arrived, out_send, out_recv).wait_recv()
    by_expert[...] = (
        jnp.dot(
            order.astype(jnp.bfloat16),
            arrived[...].reshape(total, width),
            preferred_element_type=jnp.float32,
        )
        .astype(jnp.bfloat16)
        .reshape(el, per_expert, width)
    )

    def project(e):
        load_gate(e).wait()
        load_up(e).wait()
        x = by_expert[e]
        at = pl.ds(pl.multiple_of(e * per_expert, 16), per_expert)
        partial[at, :ff] = jnp.dot(x, gate_v[e], preferred_element_type=jnp.float32)
        partial[at, ff:] = jnp.dot(x, up_v[e], preferred_element_type=jnp.float32)

    each(0, el, project)
    to_send[...] = partial[: n * share].reshape(n, share, 2 * ff).astype(jnp.bfloat16)
    each(1, n, lambda o: part_copy(o).start())
    if tilt:
        to_tilt[...] = partial[n * share :].astype(jnp.bfloat16)

        @pl.when(p == 0)
        def _():
            tilt_part.start()

    each(early, middle, send_chunk)

    each(1, n, lambda o: part_copy(o).wait_recv())

    def gather_part(o, acc):
        return acc + peers_part[o].astype(jnp.float32)

    summed = lax.fori_loop(1, n, gather_part, partial[share_of(p), :])
    hidden[share_of(p), :] = activate(summed)
    each(1, n, lambda o: hidden_copy(o, p).start())
    if tilt:

        @pl.when(p == 1)
        def _():
            tilt_part.wait_recv()
            hidden[tilted, :] = activate(partial[tilted, :] + peers_tilt[...].astype(jnp.float32))
            tilt_hidden.start()

    each(middle, own, send_chunk)
    each(1, n, lambda o: hidden_copy(o, lax.rem(p + n - o, n)).wait_recv())
    if tilt:

        @pl.when(p == 0)
        def _():
            tilt_hidden.wait_recv()


    def contract(e):
        load_down(e).wait()
        h = hidden[pl.ds(pl.multiple_of(e * per_expert, 16), per_expert), :]
        by_expert[e] = jnp.dot(h, down_v[e], preferred_element_type=jnp.float32).astype(
            jnp.bfloat16
        )

    each(0, el, contract)
    leaving[...] = (
        jnp.dot(
            order.T.astype(jnp.bfloat16),
            by_expert[...].reshape(total, width),
            preferred_element_type=jnp.float32,
        )
        .astype(jnp.bfloat16)
        .reshape(groups, slots, width)
    )
    returned[me] = leaving[me]
    spread_all(leaving, returned, ret_send, ret_recv)

    load_kept.wait()

    def keep(e):
        synced[e, pl.ds(pl.multiple_of(p * rows, 16), rows), :] = kept[e].astype(jnp.bfloat16)

    each(0, el, keep)
    blocks(leaving, returned, ret_send, ret_recv).wait_recv()
    answers = returned[...].reshape(total, width)
    high = combine.astype(jnp.bfloat16)
    rest = combine - high.astype(jnp.float32)
    mid = rest.astype(jnp.bfloat16)
    low = (rest - mid.astype(jnp.float32)).astype(jnp.bfloat16)
    mixed[...] = (
        jnp.dot(low, answers, preferred_element_type=jnp.float32)
        + jnp.dot(mid, answers, preferred_element_type=jnp.float32)
        + jnp.dot(high, answers, preferred_element_type=jnp.float32)
    ).astype(jnp.bfloat16)

    blocks(outgoing, arrived, out_send, out_recv).wait_send()
    blocks(leaving, returned, ret_send, ret_recv).wait_send()
    each(1, n, lambda o: part_copy(o).wait_send())
    each(1, n, lambda o: hidden_copy(o, p).wait_send())
    if tilt:

        @pl.when(p == 0)
        def _():
            tilt_part.wait_send()

        @pl.when(p == 1)
        def _():
            tilt_hidden.wait_send()


    def finish(i):
        sync_copy(i).wait_send()
        sync_arrival(i).wait_recv()

    each(0, own - cover, finish)

    @pl.when(core == 0)
    def _():
        pl.semaphore_signal(nearly, inc=1, device_id=(p, me + 1), device_id_type=MESH)

    each(own - cover, own, finish)

    @pl.when(core == 1)
    def _():
        pl.semaphore_wait(nearly, 1)


def store(dims, mixed, synced, mixed_out, synced_out, mark, sems):
    n, _, el, _, nsub, late = dims
    p, core = lax.axis_index("dp"), lax.rem(lax.axis_index("expert"), 2)
    rows = synced.shape[1] // n
    own = (n - 1) * el * nsub - core * late

    def local_part(e):
        part = pl.ds(pl.multiple_of(p * rows, 16), rows)
        return pltpu.make_async_copy(synced.at[e, part], synced_out.at[e, part], sems.at[e])

    def arrived_part(i):
        offset, e, r = chunk_at(dims, i)
        part = rows_of(dims, rows, lax.rem(p + n - offset, n), r)
        return pltpu.make_async_copy(synced.at[e, part], synced_out.at[e, part], sems.at[el + i])

    out = pltpu.make_async_copy(mixed, mixed_out, sems.at[sems.shape[0] - 1])
    each(0, el, lambda e: local_part(e).start())
    each(0, own, lambda i: arrived_part(i).start())
    out.start()
    mark[...] = jnp.zeros_like(mark)
    each(0, el, lambda e: local_part(e).wait())
    each(0, own, lambda i: arrived_part(i).wait())
    out.wait()


def trailing(dims, trained, mark, tail, wide, narrow, wide_sem, send_sem, recv_sem):
    n, _, el, rc, nsub, late = dims
    p, me = lax.axis_index("dp"), lax.axis_index("expert")
    width = wide.shape[2]
    first = (n - 1) * el * nsub - late

    def load(i):
        offset, e, r = chunk_at(dims, first + i)
        cols = pl.ds(pl.multiple_of(lax.rem(p + offset, n) * width, 128), width)
        return pltpu.make_async_copy(
            trained.at[e, pl.ds(pl.multiple_of(r, 16), rc), cols], wide.at[i], wide_sem.at[i]
        )

    def copy(i):
        offset, _, _ = chunk_at(dims, first + i)
        return pltpu.make_async_remote_copy(
            src_ref=narrow.at[i],
            dst_ref=tail.at[i],
            send_sem=send_sem,
            recv_sem=recv_sem,
            device_id=(lax.rem(p + offset, n), me),
            device_id_type=MESH,
        )

    def send(i):
        load(i).wait()
        narrow[i] = wide[i].astype(jnp.bfloat16)
        copy(i).start()

    @pl.when(lax.rem(me, 2) == 1)
    def _():
        barrier = pltpu.get_barrier_semaphore()
        each(
            1, n,
            lambda o: pl.semaphore_signal(
                barrier, inc=1, device_id=(lax.rem(p + o, n), me), device_id_type=MESH
            ),
        )
        each(0, late, lambda i: load(i).start())
        pl.semaphore_wait(barrier, n - 1)
        each(0, late, send)
        pltpu.make_async_remote_copy(
            src_ref=narrow,
            dst_ref=tail,
            send_sem=send_sem,
            recv_sem=recv_sem,
            device_id=(lax.rem(p + 1, n), me),
            device_id_type=MESH,
        ).wait()


def settle(dims, tail, stored, synced_out, sems):
    n, _, el, _, nsub, late = dims
    p, core = lax.axis_index("dp"), lax.rem(lax.axis_index("expert"), 2)
    rows = synced_out.shape[1] // n
    first = (n - 1) * el * nsub - late

    def part(i):
        offset, e, r = chunk_at(dims, first + i)
        source = lax.rem(p + n - offset, n)
        return pltpu.make_async_copy(
            tail.at[i], synced_out.at[e, rows_of(dims, rows, source, r)], sems.at[i]
        )

    each(0, core * late, lambda i: part(i).start())
    each(0, core * late, lambda i: part(i).wait())


def local(tokens, routes, route_weight, gate_weight, up_weight, down_weight, trained_down):
    n, groups = lax.axis_size("dp"), lax.axis_size("expert")
    tok_rows, width = tokens.shape
    el, _, ff = gate_weight.shape
    rows = trained_down.shape[1]
    slots = el * CAP
    total = groups * slots
    tilt = tilt_of(n, total)
    share = (total - tilt) // n
    fits = [
        d for d in range(16, rows + 1, 16) if rows % d == 0 and d * width * 2 <= CHUNK_BYTES
    ]
    rc = fits[-1]
    nsub = rows // rc
    chunks = n * el * nsub
    remote = chunks - el * nsub
    late = round(remote * LATE)
    dims = (n, groups, el, rc, nsub, late)
    bf16, f32 = jnp.bfloat16, jnp.float32
    inside = pl.BlockSpec(memory_space=pltpu.VMEM)
    anywhere = pl.BlockSpec(memory_space=pl.ANY)
    dma = pltpu.SemaphoreType.DMA
    routes, route_weight = routes.T, route_weight.T

    def in_vmem(x):
        return pltpu.with_memory_space_constraint(x, pltpu.VMEM)

    mixed, synced = pl.pallas_call(
        functools.partial(fused, dims),
        out_shape=(
            pltpu.VMEM((tok_rows, width), bf16),
            pltpu.VMEM((el, n * rows, width), bf16),
        ),
        in_specs=[anywhere] * 7,
        out_specs=(inside, inside),
        scratch_shapes=[
            pltpu.VMEM(tokens.shape, bf16),
            pltpu.VMEM(routes.shape, jnp.int32),
            pltpu.VMEM(route_weight.shape, f32),
            pltpu.VMEM(gate_weight.shape, bf16),
            pltpu.VMEM(up_weight.shape, bf16),
            pltpu.VMEM(down_weight.shape, bf16),
            pltpu.VMEM((remote, rc, width), f32),
            pltpu.VMEM((el, rows, width), f32),
            pltpu.VMEM((remote, rc, width), bf16),
            pltpu.VMEM((groups, slots, width), bf16),
            pltpu.VMEM((groups, slots, width), bf16),
            pltpu.VMEM((el, total // el, width), bf16),
            pltpu.VMEM((total, 2 * ff), f32),
            pltpu.VMEM((n, share, 2 * ff), bf16),
            pltpu.VMEM((n, share, 2 * ff), bf16),
            pltpu.VMEM((max(tilt, 16), 2 * ff), bf16),
            pltpu.VMEM((max(tilt, 16), 2 * ff), bf16),
            pltpu.VMEM((total, ff), bf16),
            pltpu.VMEM((groups, slots, width), bf16),
            pltpu.VMEM((groups, slots, width), bf16),
            dma((3,)),
            dma((3 * el,)),
            dma((remote,)),
            dma(()),
            dma((remote,)),
            dma((remote,)),
            dma(()),
            dma(()),
            dma((n,)),
            dma((n,)),
            dma((n,)),
            dma((n,)),
            dma(()),
            dma(()),
            dma((4,)),
            pltpu.SemaphoreType.REGULAR,
            pltpu.SemaphoreType.REGULAR,
        ],
        compiler_params=pltpu.CompilerParams(
            collective_id=0, has_side_effects=True, vmem_limit_bytes=52 * 2**20
        ),
        cost_estimate=pl.CostEstimate(
            flops=6 * total * width * ff, bytes_accessed=2**28, transcendentals=0
        ),
    )(tokens, routes, route_weight, gate_weight, up_weight, down_weight, trained_down)
    mixed, stored, mark = pl.pallas_call(
        functools.partial(store, dims),
        out_shape=(
            jax.ShapeDtypeStruct((tok_rows, width), bf16),
            jax.ShapeDtypeStruct((el, n * rows, width), bf16),
            pltpu.VMEM((8, 128), f32),
        ),
        in_specs=[inside] * 2,
        out_specs=(anywhere, anywhere, inside),
        scratch_shapes=[dma((el + remote + 1,))],
        compiler_params=pltpu.CompilerParams(vmem_limit_bytes=2**20),
    )(in_vmem(mixed), in_vmem(synced))
    tail = pl.pallas_call(
        functools.partial(trailing, dims),
        out_shape=pltpu.VMEM((late, rc, width), bf16),
        in_specs=[anywhere] * 2,
        out_specs=inside,
        scratch_shapes=[
            pltpu.VMEM((late, rc, width), f32),
            pltpu.VMEM((late, rc, width), bf16),
            dma((late,)),
            dma(()),
            dma(()),
        ],
        compiler_params=pltpu.CompilerParams(
            collective_id=1, has_side_effects=True, vmem_limit_bytes=56 * 2**20
        ),
    )(trained_down, in_vmem(mark))
    synced = pl.pallas_call(
        functools.partial(settle, dims),
        out_shape=jax.ShapeDtypeStruct((el, n * rows, width), bf16),
        in_specs=[inside, anywhere],
        out_specs=anywhere,
        scratch_shapes=[dma((late,))],
        input_output_aliases={1: 0},
        compiler_params=pltpu.CompilerParams(vmem_limit_bytes=2**20),
    )(in_vmem(tail), stored)
    return mixed, synced


def solution(mesh):
    placed = (
        P("expert", "dp"),
        P("expert", None),
        P("expert", None),
        P("expert", "dp", None),
        P("expert", "dp", None),
        P("expert", None, "dp"),
        P("expert", "dp", None),
    )
    return jax.shard_map(
        local,
        mesh=mesh,
        in_specs=placed,
        out_specs=(P("expert", "dp"), P("expert", None, "dp")),
        check_vma=False,
    )
```

```python
import functools

import jax
import jax.numpy as jnp
from jax import lax
from jax.experimental import pallas as pl
from jax.experimental.pallas import tpu as pltpu
from jax.sharding import PartitionSpec as P

CAP = 4
CHUNK_BYTES = 150_000
FIRST = 1
EARLY = 5 / 16
MIDDLE = 1 / 16
LATE = 3 / 16
COVER = 6
TILT = 8
MESH = pl.DeviceIdType.MESH


def each(start, stop, body):
    def step(i, carry):
        body(i)
        return carry

    lax.fori_loop(start, stop, step, 0)


def chunk_at(dims, i):
    n, _, el, rc, nsub, _ = dims
    offset = lax.rem(lax.div(i, el * nsub) + 1, n)
    e = lax.rem(lax.div(i, nsub), el)
    return offset, e, lax.rem(i, nsub) * rc


def tilt_of(n, total):
    return total // TILT // 16 * 16 if n == 2 else 0


def rows_of(dims, rows, source, r):
    return pl.ds(pl.multiple_of(source * rows + r, 16), dims[3])


def fused(
    dims,
    tokens, routes, route_weight, gate_weight, up_weight, down_weight, trained,
    mixed, synced,
    tok_v, routes_v, weight_v, gate_v, up_v, down_v, wide, kept, narrow,
    outgoing, arrived, by_expert, partial, to_send, peers_part, to_tilt, peers_tilt, hidden,
    leaving, returned,
    small_sem, load_sem, wide_sem, kept_sem, sync_send, sync_recv,
    out_send, out_recv, part_send, part_recv, hid_send, hid_recv, ret_send, ret_recv,
    tilt_sem, entered, nearly,
):
    n, groups, el, rc, nsub, late = dims
    p, me = lax.axis_index("dp"), lax.axis_index("expert")
    core = lax.rem(me, 2)
    rows = trained.shape[1]
    tok_rows, width = tok_v.shape
    ff = gate_v.shape[2]
    slots = el * CAP
    total = groups * slots
    tilt = tilt_of(n, total)
    share = (total - tilt) // n
    tilted = pl.ds(n * share, tilt)
    per_expert = total // el
    per_peer = el * nsub
    remote = (n - 1) * per_peer
    early = round(remote * EARLY)
    middle = early + round(remote * MIDDLE)
    own = remote - core * late
    cover = min(COVER, remote - late)

    def peer(offset):
        return lax.rem(p + offset, n)

    def share_of(device):
        return pl.ds(pl.multiple_of(device * share, 16), share)

    def load_wide(i):
        offset, e, r = chunk_at(dims, i)
        cols = pl.ds(pl.multiple_of(peer(offset) * width, 128), width)
        return pltpu.make_async_copy(
            trained.at[e, pl.ds(pl.multiple_of(r, 16), rc), cols], wide.at[i], wide_sem.at[i]
        )

    def sync_copy(i):
        offset, e, r = chunk_at(dims, i)
        return pltpu.make_async_remote_copy(
            src_ref=narrow.at[i],
            dst_ref=synced.at[e, rows_of(dims, rows, p, r), :],
            send_sem=sync_send.at[i],
            recv_sem=sync_recv.at[i],
            device_id=(peer(offset), me),
            device_id_type=MESH,
        )

    def sync_arrival(i):
        offset, e, r = chunk_at(dims, i)
        source = lax.rem(p + n - offset, n)
        return pltpu.make_async_remote_copy(
            src_ref=narrow.at[i],
            dst_ref=synced.at[e, rows_of(dims, rows, source, r), :],
            send_sem=sync_send.at[i],
            recv_sem=sync_recv.at[i],
            device_id=(peer(offset), me),
            device_id_type=MESH,
        )

    load_kept = pltpu.make_async_copy(
        trained.at[:, :, pl.ds(pl.multiple_of(p * width, 128), width)], kept, kept_sem
    )

    def send_chunk(i):
        load_wide(i).wait()
        narrow[i] = wide[i].astype(jnp.bfloat16)
        sync_copy(i).start()

    def spread(source, target, send, recv, slot):
        return pltpu.make_async_remote_copy(
            src_ref=source.at[slot],
            dst_ref=target.at[me],
            send_sem=send,
            recv_sem=recv,
            device_id=(p, slot),
            device_id_type=MESH,
        )

    def spread_all(source, target, send, recv):
        each(
            1, groups,
            lambda o: spread(source, target, send, recv, lax.rem(me + o, groups)).start(),
        )

    def blocks(source, target, send, recv):
        some = pl.ds(0, groups - 1)
        return pltpu.make_async_remote_copy(
            src_ref=source.at[some],
            dst_ref=target.at[some],
            send_sem=send,
            recv_sem=recv,
            device_id=(p, lax.rem(me + 1, groups)),
            device_id_type=MESH,
        )

    def part_copy(o):
        return pltpu.make_async_remote_copy(
            src_ref=to_send.at[peer(o)],
            dst_ref=peers_part.at[o],
            send_sem=part_send.at[o],
            recv_sem=part_recv.at[o],
            device_id=(peer(o), me),
            device_id_type=MESH,
        )

    def hidden_copy(o, origin):
        return pltpu.make_async_remote_copy(
            src_ref=hidden.at[share_of(origin), :],
            dst_ref=hidden.at[share_of(origin), :],
            send_sem=hid_send.at[o],
            recv_sem=hid_recv.at[o],
            device_id=(peer(o), me),
            device_id_type=MESH,
        )

    def tilt_copy(source, target, k, device):
        return pltpu.make_async_remote_copy(
            src_ref=source,
            dst_ref=target,
            send_sem=tilt_sem.at[k],
            recv_sem=tilt_sem.at[k + 1],
            device_id=(device, me),
            device_id_type=MESH,
        )

    if tilt:
        tilt_part = tilt_copy(to_tilt, peers_tilt, 0, 1)
        tilt_hidden = tilt_copy(hidden.at[tilted, :], hidden.at[tilted, :], 2, 0)

    def activate(summed):
        gate, up = summed[:, :ff], summed[:, ff:]
        return (gate / (1.0 + jnp.exp(-gate)) * up).astype(jnp.bfloat16)

    smalls = [
        pltpu.make_async_copy(src, dst, small_sem.at[i])
        for i, (src, dst) in enumerate(
            ((routes, routes_v), (route_weight, weight_v), (tokens, tok_v))
        )
    ]

    def weights(k, src, dst):
        return lambda e: pltpu.make_async_copy(src.at[e], dst.at[e], load_sem.at[k * el + e])

    load_gate = weights(0, gate_weight, gate_v)
    load_up = weights(1, up_weight, up_v)
    load_down = weights(2, down_weight, down_v)

    barrier = pltpu.get_barrier_semaphore()

    def greet(device):
        pl.semaphore_signal(barrier, inc=1, device_id=device, device_id_type=MESH)

    each(0, FIRST, lambda i: load_wide(i).start())
    leader = me - core
    each(1, n, lambda o: greet((peer(o), me)))

    @pl.when(core == 0)
    def _():
        greet((p, me + 1))

    @pl.when(core == 1)
    def _():
        each(0, groups // 2, lambda j: greet((p, lax.rem(leader + 2 * j, groups))))

    @pl.when(core == 0)
    def _():
        each(1, groups // 2, lambda j: greet((p, lax.rem(leader + 2 * j, groups))))

    for copy in smalls:
        copy.start()
    each(FIRST, early, lambda i: load_wide(i).start())
    each(0, el, lambda e: load_gate(e).start())
    each(0, el, lambda e: load_up(e).start())
    each(early, own, lambda i: load_wide(i).start())
    each(0, el, lambda e: load_down(e).start())
    load_kept.start()
    pl.semaphore_wait(barrier, n - 1 + jnp.where(core == 0, groups - 1, 1))

    @pl.when(core == 0)
    def _():
        pl.semaphore_signal(entered, inc=1, device_id=(p, me + 1), device_id_type=MESH)

    each(0, early, send_chunk)

    for copy in smalls:
        copy.wait()
    slot = lax.broadcasted_iota(jnp.int32, (total, tok_rows), 0)
    slot_expert = slot // CAP
    chosen = jnp.zeros((total, tok_rows), jnp.float32)
    scale = jnp.zeros((total, tok_rows), jnp.float32)
    for k in range(routes_v.shape[0]):
        hit = routes_v[k : k + 1, :] == slot_expert
        chosen = chosen + jnp.where(hit, 1.0, 0.0)
        scale = scale + jnp.where(hit, weight_v[k : k + 1, :], 0.0)
    row = lax.broadcasted_iota(jnp.int32, (tok_rows, tok_rows), 0)
    col = lax.broadcasted_iota(jnp.int32, (tok_rows, tok_rows), 1)
    before = jnp.where(row < col, 1.0, 0.0).astype(jnp.bfloat16)
    earlier = jnp.dot(chosen.astype(jnp.bfloat16), before, preferred_element_type=jnp.float32)
    placed = (chosen == 1.0) & (earlier == (slot % CAP).astype(jnp.float32))
    combine = jnp.where(placed, scale, 0.0).T
    dispatch = jnp.where(placed, 1.0, 0.0).astype(jnp.bfloat16)
    outgoing[...] = (
        jnp.dot(dispatch, tok_v[...], preferred_element_type=jnp.float32)
        .astype(jnp.bfloat16)
        .reshape(groups, slots, width)
    )
    arrived[me] = outgoing[me]

    @pl.when(core == 1)
    def _():
        pl.semaphore_wait(entered, 1)

    spread_all(outgoing, arrived, out_send, out_recv)

    r = lax.broadcasted_iota(jnp.int32, (total, total), 0)
    c = lax.broadcasted_iota(jnp.int32, (total, total), 1)
    home = ((r // CAP) % groups) * slots + (r // per_expert) * CAP + r % CAP
    order = jnp.where(c == home, 1.0, 0.0)
    blocks(outgoing, arrived, out_send, out_recv).wait_recv()
    by_expert[...] = (
        jnp.dot(
            order.astype(jnp.bfloat16),
            arrived[...].reshape(total, width),
            preferred_element_type=jnp.float32,
        )
        .astype(jnp.bfloat16)
        .reshape(el, per_expert, width)
    )

    def project(e):
        load_gate(e).wait()
        load_up(e).wait()
        x = by_expert[e]
        at = pl.ds(pl.multiple_of(e * per_expert, 16), per_expert)
        partial[at, :ff] = jnp.dot(x, gate_v[e], preferred_element_type=jnp.float32)
        partial[at, ff:] = jnp.dot(x, up_v[e], preferred_element_type=jnp.float32)

    each(0, el, project)
    to_send[...] = partial[: n * share].reshape(n, share, 2 * ff).astype(jnp.bfloat16)
    each(1, n, lambda o: part_copy(o).start())
    if tilt:
        to_tilt[...] = partial[n * share :].astype(jnp.bfloat16)

        @pl.when(p == 0)
        def _():
            tilt_part.start()

    each(early, middle, send_chunk)

    each(1, n, lambda o: part_copy(o).wait_recv())

    def gather_part(o, acc):
        return acc + peers_part[o].astype(jnp.float32)

    summed = lax.fori_loop(1, n, gather_part, partial[share_of(p), :])
    hidden[share_of(p), :] = activate(summed)
    each(1, n, lambda o: hidden_copy(o, p).start())
    if tilt:

        @pl.when(p == 1)
        def _():
            tilt_part.wait_recv()
            hidden[tilted, :] = activate(partial[tilted, :] + peers_tilt[...].astype(jnp.float32))
            tilt_hidden.start()

    each(middle, own, send_chunk)
    each(1, n, lambda o: hidden_copy(o, lax.rem(p + n - o, n)).wait_recv())
    if tilt:

        @pl.when(p == 0)
        def _():
            tilt_hidden.wait_recv()


    def contract(e):
        load_down(e).wait()
        h = hidden[pl.ds(pl.multiple_of(e * per_expert, 16), per_expert), :]
        by_expert[e] = jnp.dot(h, down_v[e], preferred_element_type=jnp.float32).astype(
            jnp.bfloat16
        )

    each(0, el, contract)
    leaving[...] = (
        jnp.dot(
            order.T.astype(jnp.bfloat16),
            by_expert[...].reshape(total, width),
            preferred_element_type=jnp.float32,
        )
        .astype(jnp.bfloat16)
        .reshape(groups, slots, width)
    )
    returned[me] = leaving[me]
    spread_all(leaving, returned, ret_send, ret_recv)

    load_kept.wait()

    def keep(e):
        synced[e, pl.ds(pl.multiple_of(p * rows, 16), rows), :] = kept[e].astype(jnp.bfloat16)

    each(0, el, keep)
    blocks(leaving, returned, ret_send, ret_recv).wait_recv()
    answers = returned[...].reshape(total, width)
    high = combine.astype(jnp.bfloat16)
    rest = combine - high.astype(jnp.float32)
    mid = rest.astype(jnp.bfloat16)
    low = (rest - mid.astype(jnp.float32)).astype(jnp.bfloat16)
    mixed[...] = (
        jnp.dot(low, answers, preferred_element_type=jnp.float32)
        + jnp.dot(mid, answers, preferred_element_type=jnp.float32)
        + jnp.dot(high, answers, preferred_element_type=jnp.float32)
    ).astype(jnp.bfloat16)

    blocks(outgoing, arrived, out_send, out_recv).wait_send()
    blocks(leaving, returned, ret_send, ret_recv).wait_send()
    each(1, n, lambda o: part_copy(o).wait_send())
    each(1, n, lambda o: hidden_copy(o, p).wait_send())
    if tilt:

        @pl.when(p == 0)
        def _():
            tilt_part.wait_send()

        @pl.when(p == 1)
        def _():
            tilt_hidden.wait_send()


    def finish(i):
        sync_copy(i).wait_send()
        sync_arrival(i).wait_recv()

    each(0, own - cover, finish)

    @pl.when(core == 0)
    def _():
        pl.semaphore_signal(nearly, inc=1, device_id=(p, me + 1), device_id_type=MESH)

    each(own - cover, own, finish)

    @pl.when(core == 1)
    def _():
        pl.semaphore_wait(nearly, 1)


def store(dims, mixed, synced, mixed_out, synced_out, mark, sems):
    n, _, el, _, nsub, late = dims
    p, core = lax.axis_index("dp"), lax.rem(lax.axis_index("expert"), 2)
    rows = synced.shape[1] // n
    own = (n - 1) * el * nsub - core * late

    def local_part(e):
        part = pl.ds(pl.multiple_of(p * rows, 16), rows)
        return pltpu.make_async_copy(synced.at[e, part], synced_out.at[e, part], sems.at[e])

    def arrived_part(i):
        offset, e, r = chunk_at(dims, i)
        part = rows_of(dims, rows, lax.rem(p + n - offset, n), r)
        return pltpu.make_async_copy(synced.at[e, part], synced_out.at[e, part], sems.at[el + i])

    out = pltpu.make_async_copy(mixed, mixed_out, sems.at[sems.shape[0] - 1])
    each(0, el, lambda e: local_part(e).start())
    each(0, own, lambda i: arrived_part(i).start())
    out.start()
    mark[...] = jnp.zeros_like(mark)
    each(0, el, lambda e: local_part(e).wait())
    each(0, own, lambda i: arrived_part(i).wait())
    out.wait()


def trailing(dims, trained, mark, tail, wide, narrow, wide_sem, send_sem, recv_sem):
    n, _, el, rc, nsub, late = dims
    p, me = lax.axis_index("dp"), lax.axis_index("expert")
    width = wide.shape[2]
    first = (n - 1) * el * nsub - late

    def load(i):
        offset, e, r = chunk_at(dims, first + i)
        cols = pl.ds(pl.multiple_of(lax.rem(p + offset, n) * width, 128), width)
        return pltpu.make_async_copy(
            trained.at[e, pl.ds(pl.multiple_of(r, 16), rc), cols], wide.at[i], wide_sem.at[i]
        )

    def copy(i):
        offset, _, _ = chunk_at(dims, first + i)
        return pltpu.make_async_remote_copy(
            src_ref=narrow.at[i],
            dst_ref=tail.at[i],
            send_sem=send_sem,
            recv_sem=recv_sem,
            device_id=(lax.rem(p + offset, n), me),
            device_id_type=MESH,
        )

    def send(i):
        load(i).wait()
        narrow[i] = wide[i].astype(jnp.bfloat16)
        copy(i).start()

    @pl.when(lax.rem(me, 2) == 1)
    def _():
        barrier = pltpu.get_barrier_semaphore()
        each(
            1, n,
            lambda o: pl.semaphore_signal(
                barrier, inc=1, device_id=(lax.rem(p + o, n), me), device_id_type=MESH
            ),
        )
        each(0, late, lambda i: load(i).start())
        pl.semaphore_wait(barrier, n - 1)
        each(0, late, send)
        pltpu.make_async_remote_copy(
            src_ref=narrow,
            dst_ref=tail,
            send_sem=send_sem,
            recv_sem=recv_sem,
            device_id=(lax.rem(p + 1, n), me),
            device_id_type=MESH,
        ).wait()


def settle(dims, tail, stored, synced_out, sems):
    n, _, el, _, nsub, late = dims
    p, core = lax.axis_index("dp"), lax.rem(lax.axis_index("expert"), 2)
    rows = synced_out.shape[1] // n
    first = (n - 1) * el * nsub - late

    def part(i):
        offset, e, r = chunk_at(dims, first + i)
        source = lax.rem(p + n - offset, n)
        return pltpu.make_async_copy(
            tail.at[i], synced_out.at[e, rows_of(dims, rows, source, r)], sems.at[i]
        )

    each(0, core * late, lambda i: part(i).start())
    each(0, core * late, lambda i: part(i).wait())


def local(tokens, routes, route_weight, gate_weight, up_weight, down_weight, trained_down):
    n, groups = lax.axis_size("dp"), lax.axis_size("expert")
    tok_rows, width = tokens.shape
    el, _, ff = gate_weight.shape
    rows = trained_down.shape[1]
    slots = el * CAP
    total = groups * slots
    tilt = tilt_of(n, total)
    share = (total - tilt) // n
    fits = [
        d for d in range(16, rows + 1, 16) if rows % d == 0 and d * width * 2 <= CHUNK_BYTES
    ]
    rc = fits[-1]
    nsub = rows // rc
    chunks = n * el * nsub
    remote = chunks - el * nsub
    late = round(remote * LATE)
    dims = (n, groups, el, rc, nsub, late)
    bf16, f32 = jnp.bfloat16, jnp.float32
    inside = pl.BlockSpec(memory_space=pltpu.VMEM)
    anywhere = pl.BlockSpec(memory_space=pl.ANY)
    dma = pltpu.SemaphoreType.DMA
    routes, route_weight = routes.T, route_weight.T

    def in_vmem(x):
        return pltpu.with_memory_space_constraint(x, pltpu.VMEM)

    mixed, synced = pl.pallas_call(
        functools.partial(fused, dims),
        out_shape=(
            pltpu.VMEM((tok_rows, width), bf16),
            pltpu.VMEM((el, n * rows, width), bf16),
        ),
        in_specs=[anywhere] * 7,
        out_specs=(inside, inside),
        scratch_shapes=[
            pltpu.VMEM(tokens.shape, bf16),
            pltpu.VMEM(routes.shape, jnp.int32),
            pltpu.VMEM(route_weight.shape, f32),
            pltpu.VMEM(gate_weight.shape, bf16),
            pltpu.VMEM(up_weight.shape, bf16),
            pltpu.VMEM(down_weight.shape, bf16),
            pltpu.VMEM((remote, rc, width), f32),
            pltpu.VMEM((el, rows, width), f32),
            pltpu.VMEM((remote, rc, width), bf16),
            pltpu.VMEM((groups, slots, width), bf16),
            pltpu.VMEM((groups, slots, width), bf16),
            pltpu.VMEM((el, total // el, width), bf16),
            pltpu.VMEM((total, 2 * ff), f32),
            pltpu.VMEM((n, share, 2 * ff), bf16),
            pltpu.VMEM((n, share, 2 * ff), bf16),
            pltpu.VMEM((max(tilt, 16), 2 * ff), bf16),
            pltpu.VMEM((max(tilt, 16), 2 * ff), bf16),
            pltpu.VMEM((total, ff), bf16),
            pltpu.VMEM((groups, slots, width), bf16),
            pltpu.VMEM((groups, slots, width), bf16),
            dma((3,)),
            dma((3 * el,)),
            dma((remote,)),
            dma(()),
            dma((remote,)),
            dma((remote,)),
            dma(()),
            dma(()),
            dma((n,)),
            dma((n,)),
            dma((n,)),
            dma((n,)),
            dma(()),
            dma(()),
            dma((4,)),
            pltpu.SemaphoreType.REGULAR,
            pltpu.SemaphoreType.REGULAR,
        ],
        compiler_params=pltpu.CompilerParams(
            collective_id=0, has_side_effects=True, vmem_limit_bytes=52 * 2**20
        ),
        cost_estimate=pl.CostEstimate(
            flops=6 * total * width * ff, bytes_accessed=2**28, transcendentals=0
        ),
    )(tokens, routes, route_weight, gate_weight, up_weight, down_weight, trained_down)
    mixed, stored, mark = pl.pallas_call(
        functools.partial(store, dims),
        out_shape=(
            jax.ShapeDtypeStruct((tok_rows, width), bf16),
            jax.ShapeDtypeStruct((el, n * rows, width), bf16),
            pltpu.VMEM((8, 128), f32),
        ),
        in_specs=[inside] * 2,
        out_specs=(anywhere, anywhere, inside),
        scratch_shapes=[dma((el + remote + 1,))],
        compiler_params=pltpu.CompilerParams(vmem_limit_bytes=2**20),
    )(in_vmem(mixed), in_vmem(synced))
    tail = pl.pallas_call(
        functools.partial(trailing, dims),
        out_shape=pltpu.VMEM((late, rc, width), bf16),
        in_specs=[anywhere] * 2,
        out_specs=inside,
        scratch_shapes=[
            pltpu.VMEM((late, rc, width), f32),
            pltpu.VMEM((late, rc, width), bf16),
            dma((late,)),
            dma(()),
            dma(()),
        ],
        compiler_params=pltpu.CompilerParams(
            collective_id=1, has_side_effects=True, vmem_limit_bytes=56 * 2**20
        ),
    )(trained_down, in_vmem(mark))
    synced = pl.pallas_call(
        functools.partial(settle, dims),
        out_shape=jax.ShapeDtypeStruct((el, n * rows, width), bf16),
        in_specs=[inside, anywhere],
        out_specs=anywhere,
        scratch_shapes=[dma((late,))],
        input_output_aliases={1: 0},
        compiler_params=pltpu.CompilerParams(vmem_limit_bytes=2**20),
    )(in_vmem(tail), stored)
    return mixed, synced


def solution(mesh):
    placed = (
        P("expert", "dp"),
        P("expert", None),
        P("expert", None),
        P("expert", "dp", None),
        P("expert", "dp", None),
        P("expert", None, "dp"),
        P("expert", "dp", None),
    )
    return jax.shard_map(
        local,
        mesh=mesh,
        in_specs=placed,
        out_specs=(P("expert", "dp"), P("expert", None, "dp")),
        check_vma=False,
    )
```
